32 devices in a mesh: samples: 8 (over z, y), groups: 4 (over x, core).
Axes of the slice: x: 2, y: 2, z: 4, core: 2. Of those that a mesh axis runs over, the one named last changes fastest.
Arguments:
- observed: bfloat16 [128, 10240], P('samples', 'groups'), may hold values from -200 to 200
- labels: int32 [10240], P('groups'), may hold values from 0 to 31, as said below
- comp_sizes: int32 [32], P('groups'), may hold values from 128 to 512, as said below
Outputs:
- whitened: bfloat16 [128, 10240], P('samples', 'groups')
The draws below stay inside these ranges and needn't reach their ends.
Inputs may be any that keep to these rules, and one draw needn't show every extreme that they name: Group g's columns (g * 2560 to (g + 1) * 2560 - 1) carry exactly the labels g * 8 to (g + 1) * 8 - 1, and label c stands on exactly comp_sizes[c] columns. `comp_sizes`: in every group one component has exactly 512 variables; components 2k and 2k + 1 (k = 0, 1, ...) together have exactly 640 variables.
All inputs are finite; a program needn't handle non-finite values. Where the reference program divides by a largest or mean magnitude, that divisor is 1e-20 or more.
Results may differ from the reference program's by a relative error of at most 0.0038.
The reference program's roundings to bfloat16 on the way count: a program that leaves them out, or rounds other values in their place, can miss the bound.
Values may be sent and summed in bfloat16 or wider, within the bound.
A program may use at most 64 MiB of HBM per device.

```python
import math
import jax
import jax.numpy as jnp
from jax import lax

CMAX = 512
ITERS = 5
LOW = 128
AVG = 320
NCG = 8
COMPS = 32
VG = 2560
V = 10240
ROWS = 128


def group_sizes(key):
    base_key = jax.random.fold_in(key, 11)
    spread_key, shuffle_key, flip_key = jax.random.split(base_key, 3)
    group_total = COMPS // NCG
    pair_total = NCG // 2
    offsets = jax.random.randint(spread_key, (group_total, pair_total), 0, AVG - LOW + 1)
    offsets = offsets.at[:, 0].set(CMAX - AVG)
    shuffle_keys = jax.random.split(shuffle_key, group_total)
    offsets = jax.vmap(jax.random.permutation)(shuffle_keys, offsets)
    flips = jax.random.randint(flip_key, (group_total, pair_total), 0, 2) * 2 - 1
    signed = offsets * flips
    paired = jnp.stack([AVG + signed, AVG - signed], axis=2)
    return paired.reshape(group_total, NCG).astype(jnp.int32)


def draw_comp_sizes(key, part):
    return group_sizes(key).reshape(COMPS).astype(jnp.int32)


def draw_labels(key, part):
    group_total = COMPS // NCG
    sizes_table = group_sizes(key)
    ends = jnp.cumsum(sizes_table, axis=1)
    positions = jnp.arange(VG, dtype=jnp.int32)
    local_label = jnp.sum((positions[None, :, None] >= ends[:, None, :]).astype(jnp.int32), axis=2)
    shuffle_keys = jax.random.split(jax.random.fold_in(key, 13), group_total)
    shuffled = jax.vmap(jax.random.permutation)(shuffle_keys, local_label)
    group_offset = jnp.arange(group_total, dtype=jnp.int32)[:, None] * NCG
    return (shuffled + group_offset).reshape(V).astype(jnp.int32)


def draw_observed(key, part):
    base_key = jax.random.fold_in(key, 17)
    noise_key, column_key, row_key = jax.random.split(base_key, 3)
    column_trend = jnp.exp(math.log(3.0) * jnp.arange(V, dtype=jnp.float32) / V)
    row_trend = jnp.exp(math.log(3.0) * jnp.arange(ROWS, dtype=jnp.float32) / ROWS)
    noise = jnp.clip(jax.random.normal(noise_key, (ROWS, V), jnp.float32), -5.0, 5.0)
    column_rough = jnp.exp(jax.random.uniform(column_key, (V,), jnp.float32, 0.0, math.log(2.0)))
    row_rough = jnp.exp(jax.random.uniform(row_key, (ROWS,), jnp.float32, 0.0, math.log(2.0)))
    values = noise * (row_trend * row_rough)[:, None] * (column_trend * column_rough)[None, :]
    return values.astype(jnp.bfloat16)


def setup_inputs(seed: int = 0) -> dict:
    keys = jax.random.split(jax.random.key(seed), 4)
    observed = draw_observed(jax.random.fold_in(keys[3], 71), 0)
    labels = draw_labels(jax.random.fold_in(keys[3], 71), 0)
    comp_sizes = draw_comp_sizes(jax.random.fold_in(keys[3], 71), 0)
    return {"observed": observed, "labels": labels, "comp_sizes": comp_sizes}


shrink = 0.2
ridge = 0.5


def newton_inverse(matrix):
    identity = jnp.eye(matrix.shape[0], dtype=jnp.float32)
    row_bound = jnp.max(jnp.sum(jnp.abs(matrix), axis=1))
    current = identity / row_bound
    for sweep_index in range(ITERS):
        product = jnp.dot(matrix, current, precision=lax.Precision.HIGHEST)
        current = jnp.dot(current, 2.0 * identity - product, precision=lax.Precision.HIGHEST)
    return current


def reference(observed, labels, comp_sizes):
    row_count, var_count = observed.shape
    wide = observed.astype(jnp.float32)
    energy = jnp.sum(jnp.square(wide))
    average = energy / (row_count * var_count)

    def handle(result, component):
        columns = jnp.nonzero(labels == component, size=CMAX, fill_value=var_count)[0].astype(jnp.int32)
        live = (columns < var_count).astype(jnp.float32)
        safe = jnp.minimum(columns, var_count - 1).astype(jnp.int32)
        slot_block = jnp.take(wide, safe, axis=1) * live[None, :]
        covariance = jnp.dot(slot_block.T, slot_block, precision=lax.Precision.HIGHEST) / row_count
        target = jnp.trace(covariance) / comp_sizes[component].astype(jnp.float32)
        diag_lift = shrink * target + ridge * average
        matrix = (1.0 - shrink) * covariance + diag_lift * jnp.eye(CMAX, dtype=jnp.float32)
        inverse = newton_inverse(matrix).astype(jnp.bfloat16).astype(jnp.float32)
        mapped = jnp.dot(slot_block, inverse, precision=lax.Precision.HIGHEST)
        return result.at[:, columns].set(mapped, mode="drop"), None

    initial = jnp.zeros(observed.shape, jnp.float32)
    finished = lax.scan(handle, initial, jnp.arange(COMPS, dtype=jnp.int32))[0]
    return finished.astype(jnp.bfloat16)
```

```python
import functools

import jax
import jax.numpy as jnp
from jax import lax
from jax.experimental import pallas as pl
from jax.experimental.pallas import tpu as pltpu
from jax.sharding import PartitionSpec as P

CMAX = 512
ITERS = 5
LANES = 128
UNROLL_LIMIT = 1024

shrink = 0.2
ridge = 0.5

BF16 = jnp.bfloat16
F32 = jnp.float32
HIGHEST = lax.Precision.HIGHEST
MESH = pl.DeviceIdType.MESH
VMEM = pl.BlockSpec(memory_space=pltpu.VMEM)


def loop(count, step, carry, unrolled):
    if unrolled:
        for i in range(count):
            carry = step(i, carry)
        return carry
    return lax.fori_loop(0, count, step, carry)


def lane_gather(values, index):
    return jnp.take_along_axis(values, index, axis=1)


def thirds(value):
    high = value.astype(BF16)
    rest = value - high.astype(F32)
    middle = rest.astype(BF16)
    low = (rest - middle.astype(F32)).astype(BF16)
    return high, middle, low


def products(lefts, right):
    extent = right.shape[0]
    high, middle, low = thirds(right)
    left_high, left_middle, left_low = thirds(jnp.concatenate(lefts, axis=0))
    pair = jnp.concatenate([high, middle], axis=1)
    main = jnp.dot(
        jnp.concatenate([left_high, left_middle], axis=1),
        jnp.concatenate([pair, pair], axis=0),
        preferred_element_type=F32,
    )
    small = jnp.dot(
        jnp.concatenate([left_high, left_low], axis=1),
        jnp.concatenate([low, high], axis=0),
        preferred_element_type=F32,
    )
    whole = (small + main[:, extent:]) + main[:, :extent]
    return [whole[i * extent : (i + 1) * extent] for i in range(len(lefts))]


def eye(extent, value):
    down = lax.broadcasted_iota(jnp.int32, (extent, extent), 0)
    across = lax.broadcasted_iota(jnp.int32, (extent, extent), 1)
    return jnp.where(down == across, jnp.broadcast_to(value, (extent, extent)), 0.0)


def scale_and_bound(samples, gram_peak, squares, size, average):
    target = squares / samples / size
    lift = shrink * target + ridge * average
    weight = (1.0 - shrink) / samples
    return weight, lift, weight * gram_peak + lift


def whiten_rows(block, turned, inner, squares, peak, size, average, out):
    samples = block.shape[0]
    weight, lift, bound = scale_and_bound(samples, peak, squares, size, average)
    inverse_bound = 1.0 / bound
    v = inner * (weight * inverse_bound)
    e = 1.0 - lift * inverse_bound
    c = jnp.ones_like(e)
    u = d = None
    for step in range(ITERS):
        lefts = [] if step == ITERS - 1 else [v] if step == 0 else [v, u]
        results = products(lefts + ([d] if step > 1 else []), v)
        if step == 0:
            d, u = eye(samples, -c), eye(samples, 2.0 * e) - v
        else:
            through = results[-1] if step > 1 else -v
            d = (1.0 + e) * d - c * u - through
            if lefts:
                u = 2.0 * e * u - results[1]
        if lefts:
            v = 2.0 * e * v - results[0]
        c = c * (1.0 + e)
        e = e * e
    mixed = sum(jnp.dot(piece, block, preferred_element_type=F32) for piece in reversed(thirds(d)))
    mixed = mixed * (weight * inverse_bound)
    width = block.shape[1]
    stacked = jnp.concatenate(thirds(mixed), axis=0)
    wide_turned = jnp.concatenate([turned] * 3, axis=1)
    inverse = jnp.dot(wide_turned, stacked, preferred_element_type=F32) * inverse_bound
    inverse = (inverse + eye(width, c * inverse_bound)).astype(BF16)
    out(jnp.dot(block, inverse, preferred_element_type=F32).astype(BF16))


def whiten_columns(block, gram_ref, current_ref, squares, peak, size, average, out):
    samples, width = block.shape
    weight, lift, bound = scale_and_bound(samples, peak, squares, size, average)
    gram_ref[...] = weight * gram_ref[...] + eye(width, lift)
    current_ref[...] = eye(width, 1.0 / bound)

    def sweep(i, carry):
        current = current_ref[...]
        product = jnp.dot(gram_ref[...], current, precision=HIGHEST, preferred_element_type=F32)
        current_ref[...] = jnp.dot(
            current, eye(width, jnp.full((1, 1), 2.0, F32)) - product, precision=HIGHEST, preferred_element_type=F32
        )
        return carry

    lax.fori_loop(0, ITERS, sweep, 0)
    out(jnp.dot(block, current_ref[...].astype(BF16), preferred_element_type=F32).astype(BF16))


def fused_kernel(
    samples_count,
    groups_count,
    entries,
    size_hbm,
    label_hbm,
    observed_hbm,
    result_ref,
    size_ref,
    label_ref,
    observed_ref,
    load_sem,
    sorted_ref,
    high_ref,
    turn_ref,
    place_ref,
    filled_ref,
    packed_ref,
    held_ref,
    done_ref,
    back_ref,
    energy_ref,
    group_ref,
    total_ref,
    all_ref,
    *rest,
):
    *work, group_send, group_recv, total_send, total_recv, out_send, out_recv, back_send, back_recv = rest
    me = lax.axis_index("samples")
    group = lax.axis_index("groups")
    _, slot_here, rows, width = packed_ref.shape
    samples = samples_count * rows
    slots = samples_count * slot_here
    tiles = sorted_ref.shape[0]
    parts = width // LANES
    unrolled = tiles * slots <= UNROLL_LIMIT
    order = sorted(range(1, samples_count), key=lambda k: abs(2 * k - samples_count))

    def ahead(k):
        return lax.rem(me + k, samples_count)

    def behind(k):
        return lax.rem(me + samples_count - k, samples_count)

    def copy(source, target, send, recv, sample, other):
        return pltpu.make_async_remote_copy(
            src_ref=source,
            dst_ref=target,
            send_sem=send,
            recv_sem=recv,
            device_id=(sample, other),
            device_id_type=MESH,
        )

    def columns(t):
        return pl.ds(t * LANES if isinstance(t, int) else pl.multiple_of(t * LANES, LANES), LANES)

    loads = [
        pltpu.make_async_copy(source, target, load_sem.at[i])
        for i, (source, target) in enumerate(
            ((label_hbm, label_ref), (observed_hbm, observed_ref), (size_hbm, size_ref))
        )
    ]
    for item in loads:
        item.start()
    barrier = pltpu.get_barrier_semaphore()
    for k in range(1, samples_count):
        pl.semaphore_signal(barrier, inc=1, device_id=(ahead(k), group), device_id_type=MESH)
    for k in range(1, groups_count):
        other = lax.rem(group + k, groups_count)
        pl.semaphore_signal(barrier, inc=1, device_id=(me, other), device_id_type=MESH)

    for item in loads:
        item.wait()

    first = group * slots
    slot = lax.broadcasted_iota(jnp.int32, (slots, LANES), 0)
    down = lax.broadcasted_iota(jnp.int32, (LANES, LANES), 0)
    across = lax.broadcasted_iota(jnp.int32, (LANES, LANES), 1)
    upto = (down <= across).astype(BF16)
    ones = jnp.ones((LANES, LANES), BF16)

    def compare(t):
        label = label_ref[pl.ds(t, 1), :] - first
        return (label == slot).astype(F32), (label < slot).astype(F32)

    def counts(equal, less):
        rank = jnp.dot(equal.astype(BF16), upto, preferred_element_type=F32) - 1.0
        count = jnp.dot(equal.astype(BF16), ones, preferred_element_type=F32)
        before = jnp.dot(less.astype(BF16), ones, preferred_element_type=F32)
        return rank, count, before

    if unrolled:
        pairs = [compare(t) for t in range(tiles)]
        stacked = counts(*(jnp.concatenate(items, axis=0) for items in zip(*pairs)))

    def sort_tile(t, carry):
        base, energy = carry
        if unrolled:
            equal = pairs[t][0]
            rank, count, before = (item[t * slots : (t + 1) * slots] for item in stacked)
        else:
            equal, less = compare(t)
            rank, count, before = counts(equal, less)
        local = jnp.sum(equal * (before + rank), axis=0, keepdims=True).astype(jnp.int32)
        whole = slot.astype(F32) * CMAX + base + rank
        place_ref[pl.ds(t, 1), :] = jnp.sum(equal * whole, axis=0, keepdims=True).astype(jnp.int32)
        block = observed_ref[:, columns(t)]
        choose = (down == local).astype(BF16)
        sorted_ref[t] = lax.dot_general(
            block, choose, (((1,), (1,)), ((), ())), preferred_element_type=F32
        )
        high_ref[t] = (base + count).astype(jnp.int32)
        turn_ref[t] = (before - base).astype(jnp.int32)
        wide = block.astype(F32)
        square = wide * wide
        for r in range(0, rows, 8):
            energy = energy + square[r : r + 8]
        return base + count, energy

    start = (jnp.zeros((slots, LANES), F32), jnp.zeros((8, LANES), F32))
    _, total = loop(tiles, sort_tile, start, unrolled)
    energy_ref[...] = total

    lane = lax.broadcasted_iota(jnp.int32, (rows, LANES), 1)

    def pack_slot(sample, h, target):
        c = sample * slot_here + h

        def add_tile(i, packed):
            t = tiles - 1 - i
            high = jnp.broadcast_to(high_ref[t, pl.ds(c, 1), :], (rows, LANES))
            turn = jnp.broadcast_to(turn_ref[t, pl.ds(c, 1), :], (rows, LANES))
            moved = lane_gather(sorted_ref[t], (lane + turn) & (LANES - 1))
            return tuple(
                jnp.where(lane + q * LANES < high, moved, packed[q])
                for q in range(parts)
            )

        zero = jnp.zeros((rows, LANES), F32)
        packed = loop(tiles, add_tile, (zero,) * parts, unrolled)
        for q in range(parts):
            target[:, q * LANES : (q + 1) * LANES] = packed[q].astype(BF16)

    group_copies = [
        copy(
            energy_ref,
            group_ref.at[k - 1],
            group_send.at[k - 1],
            group_recv.at[k - 1],
            me,
            lax.rem(group + k, groups_count),
        )
        for k in range(1, groups_count)
    ]
    out_copies = {
        k: copy(packed_ref.at[k], held_ref.at[k], out_send.at[k - 1], out_recv.at[k - 1], ahead(k), group)
        for k in order
    }
    total_copies = [
        copy(total_ref, all_ref.at[k - 1], total_send.at[k - 1], total_recv.at[k - 1], ahead(k), group)
        for k in order
    ]
    back_copies = [
        copy(done_ref.at[k], back_ref.at[me], back_send.at[k - 1], back_recv.at[me], behind(k), group)
        for k in order
    ]

    for k in order:
        for h in range(slot_here):
            pack_slot(ahead(k), h, packed_ref.at[k, h])
    pl.semaphore_wait(barrier, samples_count + groups_count - 2)
    for item in group_copies:
        item.start()
    for k in order:
        out_copies[k].start()
    for h in range(slot_here):
        pack_slot(me, h, held_ref.at[0, h])
    for item in group_copies:
        item.wait_recv()
    for k in range(groups_count - 1):
        total = total + group_ref[k]
    total_ref[...] = total
    for item in total_copies:
        item.start()
    for k in order:
        out_copies[k].wait_recv()

    average = None
    for h in range(slot_here):
        block = held_ref[:, h].reshape(samples, width)
        turned = block.T
        wide = block.astype(F32)
        squares = jnp.sum(jnp.sum(wide * wide, axis=0, keepdims=True), axis=1, keepdims=True)
        sums = jnp.zeros((1, width), F32)
        for r in range(0, width, LANES):
            part = jnp.dot(turned[r : r + LANES], block, preferred_element_type=F32)
            if work:
                work[0][r : r + LANES, :] = part
            sums = sums + jnp.sum(jnp.abs(part), axis=0, keepdims=True)
        peak = jnp.max(sums, axis=1, keepdims=True)
        if not work:
            inner = lax.dot_general(block, block, (((1,), (1,)), ((), ())), preferred_element_type=F32)
        if average is None:
            for item in total_copies:
                item.wait_recv()
            for k in range(samples_count - 1):
                total = total + all_ref[k]
            energy = jnp.sum(jnp.sum(total, axis=0, keepdims=True), axis=1, keepdims=True)
            average = energy / entries
        size = jnp.full((1, 1), size_ref[me * slot_here + h], jnp.int32).astype(F32)

        def out(value):
            done_ref[:, h] = value.reshape(samples_count, rows, width)

        if work:
            whiten_columns(block, work[0], work[1], squares, peak, size, average, out)
        else:
            whiten_rows(block, turned, inner, squares, peak, size, average, out)

    for item in back_copies:
        item.start()

    def fill(sample, source, opening):
        for h in range(slot_here):
            wide = [source[h, :, q * LANES : (q + 1) * LANES].astype(F32) for q in range(parts)]

            def fill_tile(t, carry):
                place = jnp.broadcast_to(place_ref[pl.ds(t, 1), :], (rows, LANES))
                index = place & (LANES - 1)
                tile = (place >> (LANES.bit_length() - 1)) - (sample * slot_here + h) * parts
                if opening and h == 0:
                    value = jnp.zeros((rows, LANES), F32)
                else:
                    value = filled_ref[t]
                for q in range(parts):
                    value = jnp.where(tile == q, lane_gather(wide[q], index), value)
                filled_ref[t] = value
                return carry

            loop(tiles, fill_tile, 0, unrolled)

    fill(me, done_ref.at[0], True)
    for k in reversed(order):
        copy(
            done_ref.at[k], back_ref.at[ahead(k)], back_send.at[k - 1], back_recv.at[ahead(k)], ahead(k), group
        ).wait_recv()
        fill(ahead(k), back_ref.at[ahead(k)], False)

    def finish(t, carry):
        result_ref[:, columns(t)] = filled_ref[t]
        return carry

    loop(tiles, finish, 0, unrolled)
    for item in group_copies + list(out_copies.values()) + total_copies + back_copies:
        item.wait_send()


def body(observed, labels, comp_sizes):
    rows, width = observed.shape
    slots = comp_sizes.shape[0]
    samples_count = lax.axis_size("samples")
    groups_count = lax.axis_size("groups")
    slot_here = slots // samples_count
    tiles = width // LANES
    samples = rows * samples_count
    kind = pltpu.SemaphoreType.DMA
    table = pltpu.VMEM((tiles, slots, LANES), jnp.int32)
    wide_tiles = pltpu.VMEM((tiles, rows, LANES), F32)
    blocks = pltpu.VMEM((samples_count, slot_here, rows, CMAX), BF16)
    work = [pltpu.VMEM((CMAX, CMAX), F32)] * 2 if samples >= CMAX else []
    return pl.pallas_call(
        functools.partial(
            fused_kernel, samples_count, groups_count, float(samples * width * groups_count)
        ),
        out_shape=pltpu.VMEM((rows, width), F32),
        in_specs=[pl.BlockSpec(memory_space=pltpu.HBM)] * 3,
        out_specs=VMEM,
        scratch_shapes=[
            pltpu.SMEM(comp_sizes.shape, jnp.int32),
            pltpu.VMEM((tiles, LANES), jnp.int32),
            pltpu.VMEM((rows, width), BF16),
            kind((3,)),
            wide_tiles,
            table,
            table,
            pltpu.VMEM((tiles, LANES), jnp.int32),
            wide_tiles,
            blocks,
            blocks,
            blocks,
            blocks,
            pltpu.VMEM((8, LANES), F32),
            pltpu.VMEM((groups_count - 1, 8, LANES), F32),
            pltpu.VMEM((8, LANES), F32),
            pltpu.VMEM((samples_count - 1, 8, LANES), F32),
            *work,
            kind((groups_count - 1,)),
            kind((groups_count - 1,)),
            kind((samples_count - 1,)),
            kind((samples_count - 1,)),
            kind((samples_count - 1,)),
            kind((samples_count - 1,)),
            kind((samples_count - 1,)),
            kind((samples_count,)),
        ],
        compiler_params=pltpu.CompilerParams(
            collective_id=0, has_side_effects=True, vmem_limit_bytes=56 * 2**20
        ),
        name="whiten",
    )(comp_sizes, labels.reshape(tiles, LANES), observed).astype(BF16)


def solution(mesh):
    return jax.shard_map(
        body,
        mesh=mesh,
        in_specs=(P("samples", "groups"), P("groups"), P("groups")),
        out_specs=P("samples", "groups"),
        check_vma=False,
    )
```

```python
import functools

import jax
import jax.numpy as jnp
from jax import lax
from jax.experimental import pallas as pl
from jax.experimental.pallas import tpu as pltpu
from jax.sharding import PartitionSpec as P

CMAX = 512
ITERS = 5
LANES = 128
UNROLL_LIMIT = 1024

shrink = 0.2
ridge = 0.5

BF16 = jnp.bfloat16
F32 = jnp.float32
HIGHEST = lax.Precision.HIGHEST
MESH = pl.DeviceIdType.MESH
VMEM = pl.BlockSpec(memory_space=pltpu.VMEM)


def loop(count, step, carry, unrolled):
    if unrolled:
        for i in range(count):
            carry = step(i, carry)
        return carry
    return lax.fori_loop(0, count, step, carry)


def lane_gather(values, index):
    return jnp.take_along_axis(values, index, axis=1)


def thirds(value):
    high = value.astype(BF16)
    rest = value - high.astype(F32)
    middle = rest.astype(BF16)
    low = (rest - middle.astype(F32)).astype(BF16)
    return high, middle, low


def products(lefts, right):
    extent = right.shape[0]
    high, middle, low = thirds(right)
    left_high, left_middle, left_low = thirds(jnp.concatenate(lefts, axis=0))
    pair = jnp.concatenate([high, middle], axis=1)
    main = jnp.dot(
        jnp.concatenate([left_high, left_middle], axis=1),
        jnp.concatenate([pair, pair], axis=0),
        preferred_element_type=F32,
    )
    small = jnp.dot(
        jnp.concatenate([left_high, left_low], axis=1),
        jnp.concatenate([low, high], axis=0),
        preferred_element_type=F32,
    )
    whole = (small + main[:, extent:]) + main[:, :extent]
    return [whole[i * extent : (i + 1) * extent] for i in range(len(lefts))]


def eye(extent, value):
    down = lax.broadcasted_iota(jnp.int32, (extent, extent), 0)
    across = lax.broadcasted_iota(jnp.int32, (extent, extent), 1)
    return jnp.where(down == across, jnp.broadcast_to(value, (extent, extent)), 0.0)


def scale_and_bound(samples, gram_peak, squares, size, average):
    target = squares / samples / size
    lift = shrink * target + ridge * average
    weight = (1.0 - shrink) / samples
    return weight, lift, weight * gram_peak + lift


def whiten_rows(block, turned, inner, squares, peak, size, average, out):
    samples = block.shape[0]
    weight, lift, bound = scale_and_bound(samples, peak, squares, size, average)
    inverse_bound = 1.0 / bound
    v = inner * (weight * inverse_bound)
    e = 1.0 - lift * inverse_bound
    c = jnp.ones_like(e)
    u = d = None
    for step in range(ITERS):
        lefts = [] if step == ITERS - 1 else [v] if step == 0 else [v, u]
        results = products(lefts + ([d] if step > 1 else []), v)
        if step == 0:
            d, u = eye(samples, -c), eye(samples, 2.0 * e) - v
        else:
            through = results[-1] if step > 1 else -v
            d = (1.0 + e) * d - c * u - through
            if lefts:
                u = 2.0 * e * u - results[1]
        if lefts:
            v = 2.0 * e * v - results[0]
        c = c * (1.0 + e)
        e = e * e
    mixed = sum(jnp.dot(piece, block, preferred_element_type=F32) for piece in reversed(thirds(d)))
    mixed = mixed * (weight * inverse_bound)
    width = block.shape[1]
    stacked = jnp.concatenate(thirds(mixed), axis=0)
    wide_turned = jnp.concatenate([turned] * 3, axis=1)
    inverse = jnp.dot(wide_turned, stacked, preferred_element_type=F32) * inverse_bound
    inverse = (inverse + eye(width, c * inverse_bound)).astype(BF16)
    out(jnp.dot(block, inverse, preferred_element_type=F32).astype(BF16))


def whiten_columns(block, gram_ref, current_ref, squares, peak, size, average, out):
    samples, width = block.shape
    weight, lift, bound = scale_and_bound(samples, peak, squares, size, average)
    gram_ref[...] = weight * gram_ref[...] + eye(width, lift)
    current_ref[...] = eye(width, 1.0 / bound)

    def sweep(i, carry):
        current = current_ref[...]
        product = jnp.dot(gram_ref[...], current, precision=HIGHEST, preferred_element_type=F32)
        current_ref[...] = jnp.dot(
            current, eye(width, jnp.full((1, 1), 2.0, F32)) - product, precision=HIGHEST, preferred_element_type=F32
        )
        return carry

    lax.fori_loop(0, ITERS, sweep, 0)
    out(jnp.dot(block, current_ref[...].astype(BF16), preferred_element_type=F32).astype(BF16))


def fused_kernel(
    samples_count,
    groups_count,
    entries,
    size_hbm,
    label_hbm,
    observed_hbm,
    result_ref,
    size_ref,
    label_ref,
    observed_ref,
    load_sem,
    sorted_ref,
    high_ref,
    turn_ref,
    place_ref,
    filled_ref,
    packed_ref,
    held_ref,
    done_ref,
    back_ref,
    energy_ref,
    group_ref,
    total_ref,
    all_ref,
    *rest,
):
    *work, group_send, group_recv, total_send, total_recv, out_send, out_recv, back_send, back_recv = rest
    me = lax.axis_index("samples")
    group = lax.axis_index("groups")
    _, slot_here, rows, width = packed_ref.shape
    samples = samples_count * rows
    slots = samples_count * slot_here
    tiles = sorted_ref.shape[0]
    parts = width // LANES
    unrolled = tiles * slots <= UNROLL_LIMIT
    order = sorted(range(1, samples_count), key=lambda k: abs(2 * k - samples_count))

    def ahead(k):
        return lax.rem(me + k, samples_count)

    def behind(k):
        return lax.rem(me + samples_count - k, samples_count)

    def copy(source, target, send, recv, sample, other):
        return pltpu.make_async_remote_copy(
            src_ref=source,
            dst_ref=target,
            send_sem=send,
            recv_sem=recv,
            device_id=(sample, other),
            device_id_type=MESH,
        )

    def columns(t):
        return pl.ds(t * LANES if isinstance(t, int) else pl.multiple_of(t * LANES, LANES), LANES)

    loads = [
        pltpu.make_async_copy(source, target, load_sem.at[i])
        for i, (source, target) in enumerate(
            ((label_hbm, label_ref), (observed_hbm, observed_ref), (size_hbm, size_ref))
        )
    ]
    for item in loads:
        item.start()
    barrier = pltpu.get_barrier_semaphore()
    for k in range(1, samples_count):
        pl.semaphore_signal(barrier, inc=1, device_id=(ahead(k), group), device_id_type=MESH)
    for k in range(1, groups_count):
        other = lax.rem(group + k, groups_count)
        pl.semaphore_signal(barrier, inc=1, device_id=(me, other), device_id_type=MESH)

    for item in loads:
        item.wait()

    first = group * slots
    slot = lax.broadcasted_iota(jnp.int32, (slots, LANES), 0)
    down = lax.broadcasted_iota(jnp.int32, (LANES, LANES), 0)
    across = lax.broadcasted_iota(jnp.int32, (LANES, LANES), 1)
    upto = (down <= across).astype(BF16)
    ones = jnp.ones((LANES, LANES), BF16)

    def compare(t):
        label = label_ref[pl.ds(t, 1), :] - first
        return (label == slot).astype(F32), (label < slot).astype(F32)

    def counts(equal, less):
        rank = jnp.dot(equal.astype(BF16), upto, preferred_element_type=F32) - 1.0
        count = jnp.dot(equal.astype(BF16), ones, preferred_element_type=F32)
        before = jnp.dot(less.astype(BF16), ones, preferred_element_type=F32)
        return rank, count, before

    if unrolled:
        pairs = [compare(t) for t in range(tiles)]
        stacked = counts(*(jnp.concatenate(items, axis=0) for items in zip(*pairs)))

    def sort_tile(t, carry):
        base, energy = carry
        if unrolled:
            equal = pairs[t][0]
            rank, count, before = (item[t * slots : (t + 1) * slots] for item in stacked)
        else:
            equal, less = compare(t)
            rank, count, before = counts(equal, less)
        local = jnp.sum(equal * (before + rank), axis=0, keepdims=True).astype(jnp.int32)
        whole = slot.astype(F32) * CMAX + base + rank
        place_ref[pl.ds(t, 1), :] = jnp.sum(equal * whole, axis=0, keepdims=True).astype(jnp.int32)
        block = observed_ref[:, columns(t)]
        choose = (down == local).astype(BF16)
        sorted_ref[t] = lax.dot_general(
            block, choose, (((1,), (1,)), ((), ())), preferred_element_type=F32
        )
        high_ref[t] = (base + count).astype(jnp.int32)
        turn_ref[t] = (before - base).astype(jnp.int32)
        wide = block.astype(F32)
        square = wide * wide
        for r in range(0, rows, 8):
            energy = energy + square[r : r + 8]
        return base + count, energy

    start = (jnp.zeros((slots, LANES), F32), jnp.zeros((8, LANES), F32))
    _, total = loop(tiles, sort_tile, start, unrolled)
    energy_ref[...] = total

    lane = lax.broadcasted_iota(jnp.int32, (rows, LANES), 1)

    def pack_slot(sample, h, target):
        c = sample * slot_here + h

        def add_tile(i, packed):
            t = tiles - 1 - i
            high = jnp.broadcast_to(high_ref[t, pl.ds(c, 1), :], (rows, LANES))
            turn = jnp.broadcast_to(turn_ref[t, pl.ds(c, 1), :], (rows, LANES))
            moved = lane_gather(sorted_ref[t], (lane + turn) & (LANES - 1))
            return tuple(
                jnp.where(lane + q * LANES < high, moved, packed[q])
                for q in range(parts)
            )

        zero = jnp.zeros((rows, LANES), F32)
        packed = loop(tiles, add_tile, (zero,) * parts, unrolled)
        for q in range(parts):
            target[:, q * LANES : (q + 1) * LANES] = packed[q].astype(BF16)

    group_copies = [
        copy(
            energy_ref,
            group_ref.at[k - 1],
            group_send.at[k - 1],
            group_recv.at[k - 1],
            me,
            lax.rem(group + k, groups_count),
        )
        for k in range(1, groups_count)
    ]
    out_copies = {
        k: copy(packed_ref.at[k], held_ref.at[k], out_send.at[k - 1], out_recv.at[k - 1], ahead(k), group)
        for k in order
    }
    total_copies = [
        copy(total_ref, all_ref.at[k - 1], total_send.at[k - 1], total_recv.at[k - 1], ahead(k), group)
        for k in order
    ]
    back_copies = [
        copy(done_ref.at[k], back_ref.at[me], back_send.at[k - 1], back_recv.at[me], behind(k), group)
        for k in order
    ]

    for k in order:
        for h in range(slot_here):
            pack_slot(ahead(k), h, packed_ref.at[k, h])
    pl.semaphore_wait(barrier, samples_count + groups_count - 2)
    for item in group_copies:
        item.start()
    for k in order:
        out_copies[k].start()
    for h in range(slot_here):
        pack_slot(me, h, held_ref.at[0, h])
    for item in group_copies:
        item.wait_recv()
    for k in range(groups_count - 1):
        total = total + group_ref[k]
    total_ref[...] = total
    for item in total_copies:
        item.start()
    for k in order:
        out_copies[k].wait_recv()

    average = None
    for h in range(slot_here):
        block = held_ref[:, h].reshape(samples, width)
        turned = block.T
        wide = block.astype(F32)
        squares = jnp.sum(jnp.sum(wide * wide, axis=0, keepdims=True), axis=1, keepdims=True)
        sums = jnp.zeros((1, width), F32)
        for r in range(0, width, LANES):
            part = jnp.dot(turned[r : r + LANES], block, preferred_element_type=F32)
            if work:
                work[0][r : r + LANES, :] = part
            sums = sums + jnp.sum(jnp.abs(part), axis=0, keepdims=True)
        peak = jnp.max(sums, axis=1, keepdims=True)
        if not work:
            inner = lax.dot_general(block, block, (((1,), (1,)), ((), ())), preferred_element_type=F32)
        if average is None:
            for item in total_copies:
                item.wait_recv()
            for k in range(samples_count - 1):
                total = total + all_ref[k]
            energy = jnp.sum(jnp.sum(total, axis=0, keepdims=True), axis=1, keepdims=True)
            average = energy / entries
        size = jnp.full((1, 1), size_ref[me * slot_here + h], jnp.int32).astype(F32)

        def out(value):
            done_ref[:, h] = value.reshape(samples_count, rows, width)

        if work:
            whiten_columns(block, work[0], work[1], squares, peak, size, average, out)
        else:
            whiten_rows(block, turned, inner, squares, peak, size, average, out)

    for item in back_copies:
        item.start()

    def fill(sample, source, opening):
        for h in range(slot_here):
            wide = [source[h, :, q * LANES : (q + 1) * LANES].astype(F32) for q in range(parts)]

            def fill_tile(t, carry):
                place = jnp.broadcast_to(place_ref[pl.ds(t, 1), :], (rows, LANES))
                index = place & (LANES - 1)
                tile = (place >> (LANES.bit_length() - 1)) - (sample * slot_here + h) * parts
                if opening and h == 0:
                    value = jnp.zeros((rows, LANES), F32)
                else:
                    value = filled_ref[t]
                for q in range(parts):
                    value = jnp.where(tile == q, lane_gather(wide[q], index), value)
                filled_ref[t] = value
                return carry

            loop(tiles, fill_tile, 0, unrolled)

    fill(me, done_ref.at[0], True)
    for k in reversed(order):
        copy(
            done_ref.at[k], back_ref.at[ahead(k)], back_send.at[k - 1], back_recv.at[ahead(k)], ahead(k), group
        ).wait_recv()
        fill(ahead(k), back_ref.at[ahead(k)], False)

    def finish(t, carry):
        result_ref[:, columns(t)] = filled_ref[t]
        return carry

    loop(tiles, finish, 0, unrolled)
    for item in group_copies + list(out_copies.values()) + total_copies + back_copies:
        item.wait_send()


def pieces(value):
    high = value.astype(BF16)
    return high, (value - high.astype(F32)).astype(BF16)


def stack_product(lefts, right):
    extent = right[0].shape[1]
    pair = jnp.concatenate(right, axis=1)
    left = jnp.concatenate([jnp.concatenate(item, axis=1) for item in lefts], axis=0)
    both = jnp.dot(left, jnp.concatenate([pair, pair], axis=0), preferred_element_type=F32)
    whole = both[:, extent:] + both[:, :extent]
    rows = right[0].shape[0]
    return [whole[i * rows : (i + 1) * rows] for i in range(len(lefts))]


def residual_powers(gram, peak):
    extent = gram.shape[0]
    one = eye(extent, jnp.ones((1, 1), F32))
    positive = peak > 0.0
    unit = jnp.where(positive, 1.0 / jnp.where(positive, peak, 1.0), 0.0)
    power = {1: one - gram * unit}
    cut = {1: pieces(power[1])}
    yield

    def extend(names, by):
        for name, value in zip(names, stack_product([cut[n - by] for n in names], cut[by])):
            power[name] = value
            cut[name] = pieces(value)

    extend([2], 1)
    yield
    extend([3, 4], 2)
    yield
    extend([5, 6, 7, 8], 4)
    total = {8: one + sum(power[i] for i in range(1, 8))}
    first = pieces(total[8])
    yield
    power[16], more = stack_product([cut[8], first], cut[8])
    total[16] = total[8] + more
    cut[16] = pieces(power[16])
    yield
    power[24], more = stack_product([cut[8], first], cut[16])
    total[24] = total[16] + more
    yield power, total


def residual_series(power, total, e):
    raised = {0: jnp.ones_like(e), 1: e}
    for i in (2, 3, 4, 5, 6, 7, 8):
        raised[i] = raised[i // 2] * raised[i - i // 2]
    raised[15] = raised[8] * raised[7]
    raised[16] = raised[8] * raised[8]
    raised[23] = raised[16] * raised[7]
    raised[24] = raised[16] * raised[8]
    tail = {7: raised[7]}
    for i in range(6, -1, -1):
        tail[i] = raised[i] + tail[i + 1]
    eight = tail[0]
    extent = power[1].shape[0]
    series = eye(extent, eight - raised[7])
    for i in range(1, 7):
        series = series + power[i] * (tail[i] - raised[7])
    spread = sum(power[i] * raised[i] for i in (8, 16, 24))
    rest = sum(total[i] * (eight * raised[i - 1]) for i in (8, 16, 24))
    (through,) = stack_product([pieces(spread)], pieces(series))
    whole = eight * (1.0 + raised[8]) * (1.0 + raised[16])
    return through + (series + rest), whole


def whiten_pair(block, odd, sizes, same_ref, inverse_ref, wait_average, out):
    samples, width = block.shape
    odd_bits = odd.astype(BF16)
    second = block * odd_bits
    first = block * (1.0 - odd).astype(BF16)
    both = jnp.concatenate([first, second], axis=0)
    both_turned = both.T
    turned = both_turned[:, :samples] + both_turned[:, samples:]
    inner = jnp.dot(block, both_turned, preferred_element_type=F32)
    sums = jnp.zeros((1, width), F32)
    for r in range(0, width, LANES):
        part = jnp.dot(both_turned[r : r + LANES], both, preferred_element_type=F32)
        sums = sums + jnp.sum(jnp.abs(part), axis=0, keepdims=True)
    peaks = [jnp.max(sums * side, axis=1, keepdims=True) for side in (1.0 - odd, odd)]
    grams = [inner[:, :samples], inner[:, samples:]]
    traces = []
    for gram in grams:
        kept = gram * eye(samples, jnp.ones((1, 1), F32))
        traces.append(jnp.sum(jnp.sum(kept, axis=0, keepdims=True), axis=1, keepdims=True))
    makers = [residual_powers(gram, peak) for gram, peak in zip(grams, peaks)]
    for _ in range(6):
        found = [next(maker) for maker in makers]
    average = wait_average()
    weight = (1.0 - shrink) / samples
    middles, wholes, inverse_bounds, factors = [], [], [], []
    for (power, total), peak, trace, size in zip(found, peaks, traces, sizes):
        lift = shrink * (trace / samples / size) + ridge * average
        inverse_bound = 1.0 / (weight * peak + lift)
        middle, whole = residual_series(power, total, weight * peak * inverse_bound)
        middles += pieces(middle)
        wholes.append(whole)
        inverse_bounds.append(inverse_bound)
        factors.append(weight * inverse_bound)

    def by_side(values):
        return jnp.where(odd > 0.5, values[1], values[0])

    mixed = jnp.dot(
        jnp.concatenate(middles, axis=1),
        jnp.concatenate([first, first, second, second], axis=0),
        preferred_element_type=F32,
    )
    mixed = mixed * (-by_side(factors))
    stacked = jnp.concatenate(pieces(mixed), axis=0)
    scale = by_side(inverse_bounds)
    peak_line = by_side(wholes)
    wide_turned = jnp.concatenate([turned, turned], axis=1)
    for r in range(0, width, LANES):
        part = jnp.dot(wide_turned[r : r + LANES], stacked, preferred_element_type=F32)
        line = eye(LANES, jnp.ones((1, 1), F32)) * peak_line[:, r : r + LANES]
        for q in range(0, width, LANES):
            value = part[:, q : q + LANES]
            if q == r:
                value = value + line
            value = (value * scale[:, q : q + LANES]).astype(BF16)
            inverse_ref[r : r + LANES, q : q + LANES] = value * same_ref[r : r + LANES, q : q + LANES]
    out(jnp.dot(block, inverse_ref[...], preferred_element_type=F32).astype(BF16))


def pair_kernel(
    samples_count,
    groups_count,
    entries,
    size_hbm,
    label_hbm,
    observed_hbm,
    result_ref,
    size_ref,
    label_ref,
    observed_ref,
    load_sem,
    sorted_ref,
    side_ref,
    high_ref,
    turn_ref,
    place_ref,
    packed_ref,
    held_ref,
    odd_ref,
    same_ref,
    inverse_ref,
    done_ref,
    back_ref,
    energy_ref,
    all_ref,
    total_ref,
    total_in_ref,
    energy_send,
    energy_recv,
    total_send,
    total_recv,
    out_send,
    out_recv,
    back_send,
    back_recv,
):
    me = lax.axis_index("samples")
    group = lax.axis_index("groups")
    pairs, rows, width = packed_ref.shape
    tiles = sorted_ref.shape[0]
    table_rows = high_ref.shape[1]
    parts = width // LANES
    opening = samples_count // 4
    mine = jnp.clip(me - opening, 0, pairs - 1)
    inverts = (me >= opening) & (me < opening + pairs)
    odd_group = lax.rem(group, 2)
    number = group * samples_count + me
    devices = samples_count * groups_count

    def copy(source, target, send, recv, sample, other):
        return pltpu.make_async_remote_copy(
            src_ref=source,
            dst_ref=target,
            send_sem=send,
            recv_sem=recv,
            device_id=(sample, other),
            device_id_type=MESH,
        )

    def signal(sample, other):
        pl.semaphore_signal(barrier, inc=1, device_id=(sample, other), device_id_type=MESH)

    loads = [
        pltpu.make_async_copy(source, target, load_sem.at[i])
        for i, (source, target) in enumerate(
            ((label_hbm, label_ref), (observed_hbm, observed_ref), (size_hbm, size_ref))
        )
    ]
    for item in loads:
        item.start()
    barrier = pltpu.get_barrier_semaphore()

    @pl.when(inverts)
    def _():
        for k in range(1, samples_count):
            signal(lax.rem(me + k, samples_count), group)

    @pl.when(inverts & (odd_group == 0))
    def _():
        for j in range(1, groups_count):
            for k in range(samples_count):
                signal(lax.rem(me + k, samples_count), lax.rem(group + j, groups_count))

    for item in loads:
        item.wait()

    slots = 2 * pairs
    first = group * slots
    slot = lax.broadcasted_iota(jnp.int32, (table_rows, LANES), 0)
    down = lax.broadcasted_iota(jnp.int32, (LANES, LANES), 0)
    across = lax.broadcasted_iota(jnp.int32, (LANES, LANES), 1)
    upto = (down <= across).astype(BF16)
    ones = jnp.ones((LANES, LANES), BF16)
    energy = jnp.zeros((8, LANES), F32)
    equals, lesses, blocks, sides = [], [], [], []
    for t in range(tiles):
        block = observed_ref[:, t * LANES : (t + 1) * LANES]
        wide = block.astype(F32)
        square = wide * wide
        for r in range(0, rows, 8):
            energy = energy + square[r : r + 8]
        label = label_ref[pl.ds(t, 1), :] - first
        pair = label >> 1
        equals.append((pair == slot).astype(F32))
        lesses.append((pair < slot).astype(F32))
        side = jnp.broadcast_to((label & 1).astype(F32), (rows, LANES)).astype(BF16)
        blocks.append(jnp.concatenate([block, side], axis=0))
    energy_ref[0] = jnp.sum(energy, axis=0, keepdims=True)
    all_ref[number] = energy_ref[0]
    equal_all = jnp.concatenate(equals, axis=0).astype(BF16)
    less_all = jnp.concatenate(lesses, axis=0).astype(BF16)
    ranks = jnp.dot(equal_all, upto, preferred_element_type=F32) - 1.0
    counts = jnp.dot(equal_all, ones, preferred_element_type=F32)
    befores = jnp.dot(less_all, ones, preferred_element_type=F32)
    base = jnp.zeros((table_rows, LANES), F32)
    for t in range(tiles):
        span = slice(t * table_rows, (t + 1) * table_rows)
        rank, count, before, equal = ranks[span], counts[span], befores[span], equals[t]
        local = jnp.sum(equal * (before + rank), axis=0, keepdims=True).astype(jnp.int32)
        whole = slot.astype(F32) * width + base + rank
        place_ref[pl.ds(t, 1), :] = jnp.sum(equal * whole, axis=0, keepdims=True).astype(jnp.int32)
        choose = (down == local).astype(BF16)
        ordered = lax.dot_general(blocks[t], choose, (((1,), (1,)), ((), ())), preferred_element_type=F32)
        sorted_ref[t] = ordered[:rows]
        side_ref[t] = ordered[rows : rows + 8]
        high_ref[t] = (base + count).astype(jnp.int32)
        turn_ref[t] = (before - base).astype(jnp.int32)
        base = base + count

    lane = lax.broadcasted_iota(jnp.int32, (rows, LANES), 1)

    def reach(t):
        return range(max(0, parts - tiles + t), min(parts, t + 1))

    def pack(c, source, height):
        packed = [jnp.zeros((height, LANES), F32)] * parts
        place = lane[:height]
        for t in reversed(range(tiles)):
            high = jnp.broadcast_to(high_ref[t, pl.ds(c, 1), :], (height, LANES))
            turn = jnp.broadcast_to(turn_ref[t, pl.ds(c, 1), :], (height, LANES))
            moved = lane_gather(source[t], (place + turn) & (LANES - 1))
            for q in reach(t):
                packed[q] = jnp.where(place + q * LANES < high, moved, packed[q])
        return packed

    for p in range(pairs):
        for q, value in enumerate(pack(p, sorted_ref, rows)):
            packed_ref[p, :, q * LANES : (q + 1) * LANES] = value.astype(BF16)

    out_copies = [
        copy(packed_ref.at[p], held_ref.at[me], out_send.at[p], out_recv.at[me], opening + p, group)
        for p in range(pairs)
    ]
    hubs = [(opening + p, g) for g in range(0, groups_count, 2) for p in range(pairs)]
    energy_copies = [
        copy(energy_ref.at[0], all_ref.at[number], energy_send.at[i], energy_recv, sample, other)
        for i, (sample, other) in enumerate(hubs)
    ]

    def elsewhere(sample, other=None):
        away = me != sample
        return away if other is None else away | (group != other)

    pl.semaphore_wait(barrier, len(hubs) + odd_group * pairs - inverts.astype(jnp.int32))
    for item, hub in zip(energy_copies, hubs):
        pl.when(elsewhere(*hub))(item.start)
    for p, item in enumerate(out_copies):
        pl.when(elsewhere(opening + p))(item.start)

    total_copy = copy(total_ref, total_in_ref, total_send, total_recv, me, lax.rem(group + 1, groups_count))

    @pl.when(inverts)
    def _():
        held_ref[me] = packed_ref[mine]
        odd = jnp.concatenate(pack(mine, side_ref, 8), axis=1)
        odd_ref[...] = odd
        odd_turned = jnp.concatenate([odd] * (LANES // 8), axis=0).T
        for r in range(0, width, LANES):
            for q in range(0, width, LANES):
                same = odd_turned[r : r + LANES] == jnp.broadcast_to(odd[:1, q : q + LANES], (LANES, LANES))
                same_ref[r : r + LANES, q : q + LANES] = same.astype(F32).astype(BF16)
        for k in range(1, samples_count):
            other = lax.rem(me + k, samples_count)
            copy(
                packed_ref.at[0], held_ref.at[other], out_send.at[0], out_recv.at[other], me, group
            ).wait_recv()

        def wait_average():
            @pl.when(odd_group == 0)
            def _():
                rest = all_ref.at[pl.ds(0, devices - 1)]
                copy(rest, rest, energy_send.at[0], energy_recv, me, group).wait_recv()
                total_in_ref[...] = jnp.sum(all_ref[...], axis=0)
                total_ref[...] = jnp.sum(all_ref[...], axis=0)
                total_copy.start()

            @pl.when(odd_group == 1)
            def _():
                total_copy.wait_recv()

            return jnp.sum(total_in_ref[...], axis=1, keepdims=True) / entries

        def out(value):
            done_ref[...] = value.reshape(samples_count, rows, width)

        sizes = [
            jnp.full((1, 1), size_ref[2 * mine + h], jnp.int32).astype(F32) for h in range(2)
        ]
        block = held_ref[...].reshape(samples_count * rows, width)
        whiten_pair(block, odd_ref[:1], sizes, same_ref, inverse_ref, wait_average, out)
        for k in range(1, samples_count):
            other = lax.rem(me + k, samples_count)
            copy(
                done_ref.at[other], back_ref.at[mine], back_send.at[k - 1], back_recv.at[mine], other, group
            ).start()
        back_ref[mine] = done_ref[me]

    for k in range(pairs):
        p = jnp.where(me < opening + pairs // 2, k, pairs - 1 - k)

        @pl.when(elsewhere(opening + p))
        def _():
            copy(
                done_ref.at[0], back_ref.at[p], back_send.at[0], back_recv.at[p], opening + p, group
            ).wait_recv()

        wide = [back_ref[p, :, q * LANES : (q + 1) * LANES].astype(F32) for q in range(parts)]
        for t in range(tiles):
            place = jnp.broadcast_to(place_ref[pl.ds(t, 1), :], (rows, LANES))
            index = place & (LANES - 1)
            tile = (place >> (LANES.bit_length() - 1)) - p * parts
            if k == 0:
                value = jnp.zeros((rows, LANES), F32)
            else:
                value = result_ref[:, t * LANES : (t + 1) * LANES]
            for q in reach(t):
                value = jnp.where(tile == q, lane_gather(wide[q], index), value)
            result_ref[:, t * LANES : (t + 1) * LANES] = value

    for item, hub in zip(energy_copies, hubs):
        pl.when(elsewhere(*hub))(item.wait_send)
    for p, item in enumerate(out_copies):
        pl.when(elsewhere(opening + p))(item.wait_send)
    pl.when(inverts & (odd_group == 0))(total_copy.wait_send)

    @pl.when(inverts)
    def _():
        for k in range(1, samples_count):
            other = lax.rem(me + k, samples_count)
            copy(
                done_ref.at[other], back_ref.at[mine], back_send.at[k - 1], back_recv.at[mine], other, group
            ).wait_send()


def paired(observed, labels, comp_sizes, samples_count, groups_count):
    rows, width = observed.shape
    pairs = comp_sizes.shape[0] // 2
    pair_width = width // pairs
    tiles = width // LANES
    devices = samples_count * groups_count
    table_rows = -(-pairs // 8) * 8
    kind = pltpu.SemaphoreType.DMA
    table = pltpu.VMEM((tiles, table_rows, LANES), jnp.int32)
    square = pltpu.VMEM((pair_width, pair_width), BF16)
    blocks = pltpu.VMEM((samples_count, rows, pair_width), BF16)
    kept = pltpu.VMEM((pairs, rows, pair_width), BF16)
    line = pltpu.VMEM((1, LANES), F32)
    return pl.pallas_call(
        functools.partial(
            pair_kernel, samples_count, groups_count, float(samples_count * rows * width * groups_count)
        ),
        out_shape=pltpu.VMEM((rows, width), F32),
        in_specs=[pl.BlockSpec(memory_space=pltpu.HBM)] * 3,
        out_specs=VMEM,
        scratch_shapes=[
            pltpu.SMEM(comp_sizes.shape, jnp.int32),
            pltpu.VMEM((tiles, LANES), jnp.int32),
            pltpu.VMEM((rows, width), BF16),
            kind((3,)),
            pltpu.VMEM((tiles, rows, LANES), F32),
            pltpu.VMEM((tiles, 8, LANES), F32),
            table,
            table,
            pltpu.VMEM((tiles, LANES), jnp.int32),
            kept,
            blocks,
            pltpu.VMEM((8, pair_width), F32),
            square,
            square,
            blocks,
            kept,
            pltpu.VMEM((1, 1, LANES), F32),
            pltpu.VMEM((devices, 1, LANES), F32),
            line,
            line,
            kind((pairs * groups_count // 2,)),
            kind,
            kind,
            kind,
            kind((pairs,)),
            kind((samples_count,)),
            kind((samples_count,)),
            kind((pairs,)),
        ],
        compiler_params=pltpu.CompilerParams(
            collective_id=0, has_side_effects=True, vmem_limit_bytes=56 * 2**20
        ),
        name="whiten",
    )(comp_sizes, labels.reshape(tiles, LANES), observed).astype(BF16)


def pairs_fit(rows, width, slots, samples_count, groups_count):
    return (
        slots == samples_count
        and samples_count % 4 == 0
        and groups_count % 2 == 0
        and rows * samples_count < CMAX
        and (2 * width // slots) % LANES == 0
        and rows % 16 == 0
    )


def body(observed, labels, comp_sizes):
    rows, width = observed.shape
    slots = comp_sizes.shape[0]
    samples_count = lax.axis_size("samples")
    groups_count = lax.axis_size("groups")
    if pairs_fit(rows, width, slots, samples_count, groups_count):
        return paired(observed, labels, comp_sizes, samples_count, groups_count)
    slot_here = slots // samples_count
    tiles = width // LANES
    samples = rows * samples_count
    kind = pltpu.SemaphoreType.DMA
    table = pltpu.VMEM((tiles, slots, LANES), jnp.int32)
    wide_tiles = pltpu.VMEM((tiles, rows, LANES), F32)
    blocks = pltpu.VMEM((samples_count, slot_here, rows, CMAX), BF16)
    work = [pltpu.VMEM((CMAX, CMAX), F32)] * 2 if samples >= CMAX else []
    return pl.pallas_call(
        functools.partial(
            fused_kernel, samples_count, groups_count, float(samples * width * groups_count)
        ),
        out_shape=pltpu.VMEM((rows, width), F32),
        in_specs=[pl.BlockSpec(memory_space=pltpu.HBM)] * 3,
        out_specs=VMEM,
        scratch_shapes=[
            pltpu.SMEM(comp_sizes.shape, jnp.int32),
            pltpu.VMEM((tiles, LANES), jnp.int32),
            pltpu.VMEM((rows, width), BF16),
            kind((3,)),
            wide_tiles,
            table,
            table,
            pltpu.VMEM((tiles, LANES), jnp.int32),
            wide_tiles,
            blocks,
            blocks,
            blocks,
            blocks,
            pltpu.VMEM((8, LANES), F32),
            pltpu.VMEM((groups_count - 1, 8, LANES), F32),
            pltpu.VMEM((8, LANES), F32),
            pltpu.VMEM((samples_count - 1, 8, LANES), F32),
            *work,
            kind((groups_count - 1,)),
            kind((groups_count - 1,)),
            kind((samples_count - 1,)),
            kind((samples_count - 1,)),
            kind((samples_count - 1,)),
            kind((samples_count - 1,)),
            kind((samples_count - 1,)),
            kind((samples_count,)),
        ],
        compiler_params=pltpu.CompilerParams(
            collective_id=0, has_side_effects=True, vmem_limit_bytes=56 * 2**20
        ),
        name="whiten",
    )(comp_sizes, labels.reshape(tiles, LANES), observed).astype(BF16)


def solution(mesh):
    return jax.shard_map(
        body,
        mesh=mesh,
        in_specs=(P("samples", "groups"), P("groups"), P("groups")),
        out_specs=P("samples", "groups"),
        check_vma=False,
    )
```

```python
import functools

import jax
import jax.numpy as jnp
from jax import lax
from jax.experimental import pallas as pl
from jax.experimental.pallas import tpu as pltpu
from jax.sharding import PartitionSpec as P

CMAX = 512
ITERS = 5
LANES = 128
UNROLL_LIMIT = 1024

shrink = 0.2
ridge = 0.5

BF16 = jnp.bfloat16
F32 = jnp.float32
HIGHEST = lax.Precision.HIGHEST
MESH = pl.DeviceIdType.MESH
VMEM = pl.BlockSpec(memory_space=pltpu.VMEM)


def loop(count, step, carry, unrolled):
    if unrolled:
        for i in range(count):
            carry = step(i, carry)
        return carry
    return lax.fori_loop(0, count, step, carry)


def lane_gather(values, index):
    return jnp.take_along_axis(values, index, axis=1)


def thirds(value):
    high = value.astype(BF16)
    rest = value - high.astype(F32)
    middle = rest.astype(BF16)
    low = (rest - middle.astype(F32)).astype(BF16)
    return high, middle, low


def products(lefts, right):
    extent = right.shape[0]
    high, middle, low = thirds(right)
    left_high, left_middle, left_low = thirds(jnp.concatenate(lefts, axis=0))
    pair = jnp.concatenate([high, middle], axis=1)
    main = jnp.dot(
        jnp.concatenate([left_high, left_middle], axis=1),
        jnp.concatenate([pair, pair], axis=0),
        preferred_element_type=F32,
    )
    small = jnp.dot(
        jnp.concatenate([left_high, left_low], axis=1),
        jnp.concatenate([low, high], axis=0),
        preferred_element_type=F32,
    )
    whole = (small + main[:, extent:]) + main[:, :extent]
    return [whole[i * extent : (i + 1) * extent] for i in range(len(lefts))]


def eye(extent, value):
    down = lax.broadcasted_iota(jnp.int32, (extent, extent), 0)
    across = lax.broadcasted_iota(jnp.int32, (extent, extent), 1)
    return jnp.where(down == across, jnp.broadcast_to(value, (extent, extent)), 0.0)


def scale_and_bound(samples, gram_peak, squares, size, average):
    target = squares / samples / size
    lift = shrink * target + ridge * average
    weight = (1.0 - shrink) / samples
    return weight, lift, weight * gram_peak + lift


def whiten_rows(block, turned, inner, squares, peak, size, average, out):
    samples = block.shape[0]
    weight, lift, bound = scale_and_bound(samples, peak, squares, size, average)
    inverse_bound = 1.0 / bound
    v = inner * (weight * inverse_bound)
    e = 1.0 - lift * inverse_bound
    c = jnp.ones_like(e)
    u = d = None
    for step in range(ITERS):
        lefts = [] if step == ITERS - 1 else [v] if step == 0 else [v, u]
        results = products(lefts + ([d] if step > 1 else []), v)
        if step == 0:
            d, u = eye(samples, -c), eye(samples, 2.0 * e) - v
        else:
            through = results[-1] if step > 1 else -v
            d = (1.0 + e) * d - c * u - through
            if lefts:
                u = 2.0 * e * u - results[1]
        if lefts:
            v = 2.0 * e * v - results[0]
        c = c * (1.0 + e)
        e = e * e
    mixed = sum(jnp.dot(piece, block, preferred_element_type=F32) for piece in reversed(thirds(d)))
    mixed = mixed * (weight * inverse_bound)
    width = block.shape[1]
    stacked = jnp.concatenate(thirds(mixed), axis=0)
    wide_turned = jnp.concatenate([turned] * 3, axis=1)
    inverse = jnp.dot(wide_turned, stacked, preferred_element_type=F32) * inverse_bound
    inverse = (inverse + eye(width, c * inverse_bound)).astype(BF16)
    out(jnp.dot(block, inverse, preferred_element_type=F32).astype(BF16))


def whiten_columns(block, gram_ref, current_ref, squares, peak, size, average, out):
    samples, width = block.shape
    weight, lift, bound = scale_and_bound(samples, peak, squares, size, average)
    gram_ref[...] = weight * gram_ref[...] + eye(width, lift)
    current_ref[...] = eye(width, 1.0 / bound)

    def sweep(i, carry):
        current = current_ref[...]
        product = jnp.dot(gram_ref[...], current, precision=HIGHEST, preferred_element_type=F32)
        current_ref[...] = jnp.dot(
            current, eye(width, jnp.full((1, 1), 2.0, F32)) - product, precision=HIGHEST, preferred_element_type=F32
        )
        return carry

    lax.fori_loop(0, ITERS, sweep, 0)
    out(jnp.dot(block, current_ref[...].astype(BF16), preferred_element_type=F32).astype(BF16))


def fused_kernel(
    samples_count,
    groups_count,
    entries,
    size_hbm,
    label_hbm,
    observed_hbm,
    result_ref,
    size_ref,
    label_ref,
    observed_ref,
    load_sem,
    sorted_ref,
    high_ref,
    turn_ref,
    place_ref,
    filled_ref,
    packed_ref,
    held_ref,
    done_ref,
    back_ref,
    energy_ref,
    group_ref,
    total_ref,
    all_ref,
    *rest,
):
    *work, group_send, group_recv, total_send, total_recv, out_send, out_recv, back_send, back_recv = rest
    me = lax.axis_index("samples")
    group = lax.axis_index("groups")
    _, slot_here, rows, width = packed_ref.shape
    samples = samples_count * rows
    slots = samples_count * slot_here
    tiles = sorted_ref.shape[0]
    parts = width // LANES
    unrolled = tiles * slots <= UNROLL_LIMIT
    order = sorted(range(1, samples_count), key=lambda k: abs(2 * k - samples_count))

    def ahead(k):
        return lax.rem(me + k, samples_count)

    def behind(k):
        return lax.rem(me + samples_count - k, samples_count)

    def copy(source, target, send, recv, sample, other):
        return pltpu.make_async_remote_copy(
            src_ref=source,
            dst_ref=target,
            send_sem=send,
            recv_sem=recv,
            device_id=(sample, other),
            device_id_type=MESH,
        )

    def columns(t):
        return pl.ds(t * LANES if isinstance(t, int) else pl.multiple_of(t * LANES, LANES), LANES)

    loads = [
        pltpu.make_async_copy(source, target, load_sem.at[i])
        for i, (source, target) in enumerate(
            ((label_hbm, label_ref), (observed_hbm, observed_ref), (size_hbm, size_ref))
        )
    ]
    for item in loads:
        item.start()
    barrier = pltpu.get_barrier_semaphore()
    for k in range(1, samples_count):
        pl.semaphore_signal(barrier, inc=1, device_id=(ahead(k), group), device_id_type=MESH)
    for k in range(1, groups_count):
        other = lax.rem(group + k, groups_count)
        pl.semaphore_signal(barrier, inc=1, device_id=(me, other), device_id_type=MESH)

    for item in loads:
        item.wait()

    first = group * slots
    slot = lax.broadcasted_iota(jnp.int32, (slots, LANES), 0)
    down = lax.broadcasted_iota(jnp.int32, (LANES, LANES), 0)
    across = lax.broadcasted_iota(jnp.int32, (LANES, LANES), 1)
    upto = (down <= across).astype(BF16)
    ones = jnp.ones((LANES, LANES), BF16)

    def compare(t):
        label = label_ref[pl.ds(t, 1), :] - first
        return (label == slot).astype(F32), (label < slot).astype(F32)

    def counts(equal, less):
        rank = jnp.dot(equal.astype(BF16), upto, preferred_element_type=F32) - 1.0
        count = jnp.dot(equal.astype(BF16), ones, preferred_element_type=F32)
        before = jnp.dot(less.astype(BF16), ones, preferred_element_type=F32)
        return rank, count, before

    if unrolled:
        pairs = [compare(t) for t in range(tiles)]
        stacked = counts(*(jnp.concatenate(items, axis=0) for items in zip(*pairs)))

    def sort_tile(t, carry):
        base, energy = carry
        if unrolled:
            equal = pairs[t][0]
            rank, count, before = (item[t * slots : (t + 1) * slots] for item in stacked)
        else:
            equal, less = compare(t)
            rank, count, before = counts(equal, less)
        local = jnp.sum(equal * (before + rank), axis=0, keepdims=True).astype(jnp.int32)
        whole = slot.astype(F32) * CMAX + base + rank
        place_ref[pl.ds(t, 1), :] = jnp.sum(equal * whole, axis=0, keepdims=True).astype(jnp.int32)
        block = observed_ref[:, columns(t)]
        choose = (down == local).astype(BF16)
        sorted_ref[t] = lax.dot_general(
            block, choose, (((1,), (1,)), ((), ())), preferred_element_type=F32
        )
        high_ref[t] = (base + count).astype(jnp.int32)
        turn_ref[t] = (before - base).astype(jnp.int32)
        wide = block.astype(F32)
        square = wide * wide
        for r in range(0, rows, 8):
            energy = energy + square[r : r + 8]
        return base + count, energy

    start = (jnp.zeros((slots, LANES), F32), jnp.zeros((8, LANES), F32))
    _, total = loop(tiles, sort_tile, start, unrolled)
    energy_ref[...] = total

    lane = lax.broadcasted_iota(jnp.int32, (rows, LANES), 1)

    def pack_slot(sample, h, target):
        c = sample * slot_here + h

        def add_tile(i, packed):
            t = tiles - 1 - i
            high = jnp.broadcast_to(high_ref[t, pl.ds(c, 1), :], (rows, LANES))
            turn = jnp.broadcast_to(turn_ref[t, pl.ds(c, 1), :], (rows, LANES))
            moved = lane_gather(sorted_ref[t], (lane + turn) & (LANES - 1))
            return tuple(
                jnp.where(lane + q * LANES < high, moved, packed[q])
                for q in range(parts)
            )

        zero = jnp.zeros((rows, LANES), F32)
        packed = loop(tiles, add_tile, (zero,) * parts, unrolled)
        for q in range(parts):
            target[:, q * LANES : (q + 1) * LANES] = packed[q].astype(BF16)

    group_copies = [
        copy(
            energy_ref,
            group_ref.at[k - 1],
            group_send.at[k - 1],
            group_recv.at[k - 1],
            me,
            lax.rem(group + k, groups_count),
        )
        for k in range(1, groups_count)
    ]
    out_copies = {
        k: copy(packed_ref.at[k], held_ref.at[k], out_send.at[k - 1], out_recv.at[k - 1], ahead(k), group)
        for k in order
    }
    total_copies = [
        copy(total_ref, all_ref.at[k - 1], total_send.at[k - 1], total_recv.at[k - 1], ahead(k), group)
        for k in order
    ]
    back_copies = [
        copy(done_ref.at[k], back_ref.at[me], back_send.at[k - 1], back_recv.at[me], behind(k), group)
        for k in order
    ]

    for k in order:
        for h in range(slot_here):
            pack_slot(ahead(k), h, packed_ref.at[k, h])
    pl.semaphore_wait(barrier, samples_count + groups_count - 2)
    for item in group_copies:
        item.start()
    for k in order:
        out_copies[k].start()
    for h in range(slot_here):
        pack_slot(me, h, held_ref.at[0, h])
    for item in group_copies:
        item.wait_recv()
    for k in range(groups_count - 1):
        total = total + group_ref[k]
    total_ref[...] = total
    for item in total_copies:
        item.start()
    for k in order:
        out_copies[k].wait_recv()

    average = None
    for h in range(slot_here):
        block = held_ref[:, h].reshape(samples, width)
        turned = block.T
        wide = block.astype(F32)
        squares = jnp.sum(jnp.sum(wide * wide, axis=0, keepdims=True), axis=1, keepdims=True)
        sums = jnp.zeros((1, width), F32)
        for r in range(0, width, LANES):
            part = jnp.dot(turned[r : r + LANES], block, preferred_element_type=F32)
            if work:
                work[0][r : r + LANES, :] = part
            sums = sums + jnp.sum(jnp.abs(part), axis=0, keepdims=True)
        peak = jnp.max(sums, axis=1, keepdims=True)
        if not work:
            inner = lax.dot_general(block, block, (((1,), (1,)), ((), ())), preferred_element_type=F32)
        if average is None:
            for item in total_copies:
                item.wait_recv()
            for k in range(samples_count - 1):
                total = total + all_ref[k]
            energy = jnp.sum(jnp.sum(total, axis=0, keepdims=True), axis=1, keepdims=True)
            average = energy / entries
        size = jnp.full((1, 1), size_ref[me * slot_here + h], jnp.int32).astype(F32)

        def out(value):
            done_ref[:, h] = value.reshape(samples_count, rows, width)

        if work:
            whiten_columns(block, work[0], work[1], squares, peak, size, average, out)
        else:
            whiten_rows(block, turned, inner, squares, peak, size, average, out)

    for item in back_copies:
        item.start()

    def fill(sample, source, opening):
        for h in range(slot_here):
            wide = [source[h, :, q * LANES : (q + 1) * LANES].astype(F32) for q in range(parts)]

            def fill_tile(t, carry):
                place = jnp.broadcast_to(place_ref[pl.ds(t, 1), :], (rows, LANES))
                index = place & (LANES - 1)
                tile = (place >> (LANES.bit_length() - 1)) - (sample * slot_here + h) * parts
                if opening and h == 0:
                    value = jnp.zeros((rows, LANES), F32)
                else:
                    value = filled_ref[t]
                for q in range(parts):
                    value = jnp.where(tile == q, lane_gather(wide[q], index), value)
                filled_ref[t] = value
                return carry

            loop(tiles, fill_tile, 0, unrolled)

    fill(me, done_ref.at[0], True)
    for k in reversed(order):
        copy(
            done_ref.at[k], back_ref.at[ahead(k)], back_send.at[k - 1], back_recv.at[ahead(k)], ahead(k), group
        ).wait_recv()
        fill(ahead(k), back_ref.at[ahead(k)], False)

    def finish(t, carry):
        result_ref[:, columns(t)] = filled_ref[t]
        return carry

    loop(tiles, finish, 0, unrolled)
    for item in group_copies + list(out_copies.values()) + total_copies + back_copies:
        item.wait_send()


def pieces(value):
    high = value.astype(BF16)
    return high, (value - high.astype(F32)).astype(BF16)


def stack_product(lefts, right):
    extent = right[0].shape[1]
    pair = jnp.concatenate(right, axis=1)
    left = jnp.concatenate([jnp.concatenate(item, axis=1) for item in lefts], axis=0)
    both = jnp.dot(left, jnp.concatenate([pair, pair], axis=0), preferred_element_type=F32)
    whole = both[:, extent:] + both[:, :extent]
    rows = right[0].shape[0]
    return [whole[i * rows : (i + 1) * rows] for i in range(len(lefts))]


def residual_series(gram, peak, box):
    extent = gram.shape[0]
    one = eye(extent, jnp.ones((1, 1), F32))
    positive = peak > 0.0
    unit = jnp.where(positive, 1.0 / jnp.where(positive, peak, 1.0), 0.0)
    first = one - gram * unit
    cut = pieces(first)
    (second,) = stack_product([cut], cut)
    cut_second = pieces(second)
    yield
    third, power = stack_product([cut, cut_second], cut_second)
    yield
    e = box[0]
    square = e * e
    count = 1.0 + e
    series = one * (count + square) + first * (e + square) + second * square
    total = (one + first) + (second + third)
    count = count * (1.0 + square)
    before, raised = e * square, square * square
    yield
    for _ in range(2):
        cut = pieces(power)
        power, through, more = stack_product([cut, pieces(series), pieces(total)], cut)
        series = series + through * raised + total * (before * count)
        total = total + more
        count = count * (1.0 + raised)
        before, raised = before * raised, raised * raised
        yield
    (through,) = stack_product([pieces(series)], pieces(power))
    yield series + through * raised + total * (before * count), count * (1.0 + raised)


def whiten_pair(block, odd, sizes, same_ref, inverse_ref, share_total, wait_average, out):
    samples, width = block.shape
    odd_bits = odd.astype(BF16)
    second = block * odd_bits
    first = block * (1.0 - odd).astype(BF16)
    both = jnp.concatenate([first, second], axis=0)
    both_turned = both.T
    turned = both_turned[:, :samples] + both_turned[:, samples:]
    inner = jnp.dot(block, both_turned, preferred_element_type=F32)
    sums = jnp.zeros((1, width), F32)
    for r in range(0, width, LANES):
        part = jnp.dot(both_turned[r : r + LANES], both, preferred_element_type=F32)
        sums = sums + jnp.sum(jnp.abs(part), axis=0, keepdims=True)
    peaks = [jnp.max(sums * side, axis=1, keepdims=True) for side in (1.0 - odd, odd)]
    grams = [inner[:, :samples], inner[:, samples:]]
    traces = []
    for gram in grams:
        kept = gram * eye(samples, jnp.ones((1, 1), F32))
        traces.append(jnp.sum(jnp.sum(kept, axis=0, keepdims=True), axis=1, keepdims=True))
    share_total()
    boxes = [[], []]
    makers = [residual_series(gram, peak, box) for gram, peak, box in zip(grams, peaks, boxes)]
    for _ in range(2):
        for maker in makers:
            next(maker)
    average = wait_average()
    weight = (1.0 - shrink) / samples
    inverse_bounds = []
    for peak, trace, size, box in zip(peaks, traces, sizes, boxes):
        lift = shrink * (trace / samples / size) + ridge * average
        inverse_bound = 1.0 / (weight * peak + lift)
        box.append(weight * peak * inverse_bound)
        inverse_bounds.append(inverse_bound)
    for _ in range(4):
        found = [next(maker) for maker in makers]
    middles = [piece for middle, _ in found for piece in pieces(middle)]
    wholes = [whole for _, whole in found]
    factors = [weight * inverse_bound for inverse_bound in inverse_bounds]

    def by_side(values):
        return jnp.where(odd > 0.5, values[1], values[0])

    mixed = jnp.dot(
        jnp.concatenate(middles, axis=1),
        jnp.concatenate([first, first, second, second], axis=0),
        preferred_element_type=F32,
    )
    mixed = mixed * (-by_side(factors))
    stacked = jnp.concatenate(pieces(mixed), axis=0)
    scale = by_side(inverse_bounds)
    peak_line = by_side(wholes)
    wide_turned = jnp.concatenate([turned, turned], axis=1)
    for r in range(0, width, LANES):
        part = jnp.dot(wide_turned[r : r + LANES], stacked, preferred_element_type=F32)
        line = eye(LANES, jnp.ones((1, 1), F32)) * peak_line[:, r : r + LANES]
        for q in range(0, width, LANES):
            value = part[:, q : q + LANES]
            if q == r:
                value = value + line
            value = (value * scale[:, q : q + LANES]).astype(BF16)
            inverse_ref[r : r + LANES, q : q + LANES] = value * same_ref[r : r + LANES, q : q + LANES]
    out(jnp.dot(block, inverse_ref[...], preferred_element_type=F32).astype(BF16))


def pair_kernel(
    samples_count,
    groups_count,
    entries,
    size_hbm,
    label_hbm,
    observed_hbm,
    result_ref,
    size_ref,
    label_ref,
    observed_ref,
    load_sem,
    sorted_ref,
    side_ref,
    high_ref,
    turn_ref,
    place_ref,
    packed_ref,
    held_ref,
    odd_ref,
    same_ref,
    inverse_ref,
    done_ref,
    back_ref,
    energy_ref,
    all_ref,
    total_ref,
    total_in_ref,
    energy_send,
    energy_recv,
    total_send,
    total_recv,
    out_send,
    out_recv,
    back_send,
    back_recv,
):
    me = lax.axis_index("samples")
    group = lax.axis_index("groups")
    pairs, rows, width = packed_ref.shape
    tiles = sorted_ref.shape[0]
    table_rows = high_ref.shape[1]
    parts = width // LANES
    opening = samples_count // 4
    mine = jnp.clip(me - opening, 0, pairs - 1)
    inverts = (me >= opening) & (me < opening + pairs)
    hub_group = group == 0
    later = jnp.minimum(group, 1)
    number = group * samples_count + me
    devices = samples_count * groups_count

    def copy(source, target, send, recv, sample, other):
        return pltpu.make_async_remote_copy(
            src_ref=source,
            dst_ref=target,
            send_sem=send,
            recv_sem=recv,
            device_id=(sample, other),
            device_id_type=MESH,
        )

    def signal(sample, other):
        pl.semaphore_signal(barrier, inc=1, device_id=(sample, other), device_id_type=MESH)

    loads = [
        pltpu.make_async_copy(source, target, load_sem.at[i])
        for i, (source, target) in enumerate(
            ((label_hbm, label_ref), (observed_hbm, observed_ref), (size_hbm, size_ref))
        )
    ]
    for item in loads:
        item.start()
    barrier = pltpu.get_barrier_semaphore()

    @pl.when(inverts)
    def _():
        for k in range(1, samples_count):
            signal(lax.rem(me + k, samples_count), group)

    @pl.when(inverts & hub_group)
    def _():
        for j in range(1, groups_count):
            for k in range(samples_count):
                signal(lax.rem(me + k, samples_count), lax.rem(group + j, groups_count))

    for item in loads:
        item.wait()

    slots = 2 * pairs
    first = group * slots
    slot = lax.broadcasted_iota(jnp.int32, (table_rows, LANES), 0)
    down = lax.broadcasted_iota(jnp.int32, (LANES, LANES), 0)
    across = lax.broadcasted_iota(jnp.int32, (LANES, LANES), 1)
    upto = (down <= across).astype(BF16)
    ones = jnp.ones((LANES, LANES), BF16)
    energy = jnp.zeros((8, LANES), F32)
    equals, lesses, blocks, sides = [], [], [], []
    for t in range(tiles):
        block = observed_ref[:, t * LANES : (t + 1) * LANES]
        wide = block.astype(F32)
        square = wide * wide
        for r in range(0, rows, 8):
            energy = energy + square[r : r + 8]
        label = label_ref[pl.ds(t, 1), :] - first
        pair = label >> 1
        equals.append((pair == slot).astype(F32))
        lesses.append((pair < slot).astype(F32))
        side = jnp.broadcast_to((label & 1).astype(F32), (rows, LANES)).astype(BF16)
        blocks.append(jnp.concatenate([block, side], axis=0))
    energy_ref[0] = jnp.sum(energy, axis=0, keepdims=True)
    all_ref[number] = energy_ref[0]
    equal_all = jnp.concatenate(equals, axis=0).astype(BF16)
    less_all = jnp.concatenate(lesses, axis=0).astype(BF16)
    ranks = jnp.dot(equal_all, upto, preferred_element_type=F32) - 1.0
    counts = jnp.dot(equal_all, ones, preferred_element_type=F32)
    befores = jnp.dot(less_all, ones, preferred_element_type=F32)
    base = jnp.zeros((table_rows, LANES), F32)
    for t in range(tiles):
        span = slice(t * table_rows, (t + 1) * table_rows)
        rank, count, before, equal = ranks[span], counts[span], befores[span], equals[t]
        local = jnp.sum(equal * (before + rank), axis=0, keepdims=True).astype(jnp.int32)
        whole = slot.astype(F32) * width + base + rank
        place_ref[pl.ds(t, 1), :] = jnp.sum(equal * whole, axis=0, keepdims=True).astype(jnp.int32)
        choose = (down == local).astype(BF16)
        ordered = lax.dot_general(blocks[t], choose, (((1,), (1,)), ((), ())), preferred_element_type=F32)
        sorted_ref[t] = ordered[:rows]
        side_ref[t] = ordered[rows : rows + 8]
        high_ref[t] = (base + count).astype(jnp.int32)
        turn_ref[t] = (before - base).astype(jnp.int32)
        base = base + count

    lane = lax.broadcasted_iota(jnp.int32, (rows, LANES), 1)

    def reach(t):
        return range(max(0, parts - tiles + t), min(parts, t + 1))

    def pack(c, source, height):
        packed = [jnp.zeros((height, LANES), F32)] * parts
        place = lane[:height]
        for t in reversed(range(tiles)):
            high = jnp.broadcast_to(high_ref[t, pl.ds(c, 1), :], (height, LANES))
            turn = jnp.broadcast_to(turn_ref[t, pl.ds(c, 1), :], (height, LANES))
            moved = lane_gather(source[t], (place + turn) & (LANES - 1))
            for q in reach(t):
                packed[q] = jnp.where(place + q * LANES < high, moved, packed[q])
        return packed

    for p in range(pairs):
        for q, value in enumerate(pack(p, sorted_ref, rows)):
            packed_ref[p, :, q * LANES : (q + 1) * LANES] = value.astype(BF16)

    out_copies = [
        copy(packed_ref.at[p], held_ref.at[me], out_send.at[p], out_recv.at[me], opening + p, group)
        for p in range(pairs)
    ]
    hubs = [(opening + p, 0) for p in range(pairs)]
    energy_copies = [
        copy(energy_ref.at[0], all_ref.at[number], energy_send.at[i], energy_recv, sample, other)
        for i, (sample, other) in enumerate(hubs)
    ]

    def elsewhere(sample, other=None):
        away = me != sample
        return away if other is None else away | (group != other)

    pl.semaphore_wait(barrier, (1 + later) * pairs - inverts.astype(jnp.int32))
    for item, hub in zip(energy_copies, hubs):
        pl.when(elsewhere(*hub))(item.start)
    for p, item in enumerate(out_copies):
        pl.when(elsewhere(opening + p))(item.start)

    total_copies = [
        copy(total_ref, total_in_ref, total_send.at[g - 1], total_recv, me, g) for g in range(1, groups_count)
    ]

    @pl.when(inverts)
    def _():
        held_ref[me] = packed_ref[mine]
        odd = jnp.concatenate(pack(mine, side_ref, 8), axis=1)
        odd_ref[...] = odd
        odd_turned = jnp.concatenate([odd] * (LANES // 8), axis=0).T
        for r in range(0, width, LANES):
            for q in range(0, width, LANES):
                same = odd_turned[r : r + LANES] == jnp.broadcast_to(odd[:1, q : q + LANES], (LANES, LANES))
                same_ref[r : r + LANES, q : q + LANES] = same.astype(F32).astype(BF16)
        for k in range(1, samples_count):
            other = lax.rem(me + k, samples_count)
            copy(
                packed_ref.at[0], held_ref.at[other], out_send.at[0], out_recv.at[other], me, group
            ).wait_recv()

        def share_total():
            @pl.when(hub_group)
            def _():
                rest = all_ref.at[pl.ds(0, devices - 1)]
                copy(rest, rest, energy_send.at[0], energy_recv, me, group).wait_recv()
                total_in_ref[...] = jnp.sum(all_ref[...], axis=0)
                total_ref[...] = jnp.sum(all_ref[...], axis=0)
                for item in total_copies:
                    item.start()

        def wait_average():
            @pl.when(group != 0)
            def _():
                total_copies[0].wait_recv()

            return jnp.sum(total_in_ref[...], axis=1, keepdims=True) / entries

        def out(value):
            done_ref[...] = value.reshape(samples_count, rows, width)

        sizes = [
            jnp.full((1, 1), size_ref[2 * mine + h], jnp.int32).astype(F32) for h in range(2)
        ]
        block = held_ref[...].reshape(samples_count * rows, width)
        whiten_pair(block, odd_ref[:1], sizes, same_ref, inverse_ref, share_total, wait_average, out)
        for k in range(1, samples_count):
            other = lax.rem(me + k, samples_count)
            copy(
                done_ref.at[other], back_ref.at[mine], back_send.at[k - 1], back_recv.at[mine], other, group
            ).start()
        back_ref[mine] = done_ref[me]

    for k in range(pairs):
        p = jnp.where(me < opening + pairs // 2, k, pairs - 1 - k)

        @pl.when(elsewhere(opening + p))
        def _():
            copy(
                done_ref.at[0], back_ref.at[p], back_send.at[0], back_recv.at[p], opening + p, group
            ).wait_recv()

        wide = [back_ref[p, :, q * LANES : (q + 1) * LANES].astype(F32) for q in range(parts)]
        for t in range(tiles):
            place = jnp.broadcast_to(place_ref[pl.ds(t, 1), :], (rows, LANES))
            index = place & (LANES - 1)
            tile = (place >> (LANES.bit_length() - 1)) - p * parts
            if k == 0:
                value = jnp.zeros((rows, LANES), F32)
            else:
                value = result_ref[:, t * LANES : (t + 1) * LANES]
            for q in reach(t):
                value = jnp.where(tile == q, lane_gather(wide[q], index), value)
            result_ref[:, t * LANES : (t + 1) * LANES] = value

    for item, hub in zip(energy_copies, hubs):
        pl.when(elsewhere(*hub))(item.wait_send)
    for p, item in enumerate(out_copies):
        pl.when(elsewhere(opening + p))(item.wait_send)

    @pl.when(inverts & hub_group)
    def _():
        for item in total_copies:
            item.wait_send()


    @pl.when(inverts)
    def _():
        for k in range(1, samples_count):
            other = lax.rem(me + k, samples_count)
            copy(
                done_ref.at[other], back_ref.at[mine], back_send.at[k - 1], back_recv.at[mine], other, group
            ).wait_send()


def paired(observed, labels, comp_sizes, samples_count, groups_count):
    rows, width = observed.shape
    pairs = comp_sizes.shape[0] // 2
    pair_width = width // pairs
    tiles = width // LANES
    devices = samples_count * groups_count
    table_rows = -(-pairs // 8) * 8
    kind = pltpu.SemaphoreType.DMA
    table = pltpu.VMEM((tiles, table_rows, LANES), jnp.int32)
    square = pltpu.VMEM((pair_width, pair_width), BF16)
    blocks = pltpu.VMEM((samples_count, rows, pair_width), BF16)
    kept = pltpu.VMEM((pairs, rows, pair_width), BF16)
    line = pltpu.VMEM((1, LANES), F32)
    return pl.pallas_call(
        functools.partial(
            pair_kernel, samples_count, groups_count, float(samples_count * rows * width * groups_count)
        ),
        out_shape=pltpu.VMEM((rows, width), F32),
        in_specs=[pl.BlockSpec(memory_space=pltpu.HBM)] * 3,
        out_specs=VMEM,
        scratch_shapes=[
            pltpu.SMEM(comp_sizes.shape, jnp.int32),
            pltpu.VMEM((tiles, LANES), jnp.int32),
            pltpu.VMEM((rows, width), BF16),
            kind((3,)),
            pltpu.VMEM((tiles, rows, LANES), F32),
            pltpu.VMEM((tiles, 8, LANES), F32),
            table,
            table,
            pltpu.VMEM((tiles, LANES), jnp.int32),
            kept,
            blocks,
            pltpu.VMEM((8, pair_width), F32),
            square,
            square,
            blocks,
            kept,
            pltpu.VMEM((1, 1, LANES), F32),
            pltpu.VMEM((devices, 1, LANES), F32),
            line,
            line,
            kind((pairs,)),
            kind,
            kind((groups_count - 1,)),
            kind,
            kind((pairs,)),
            kind((samples_count,)),
            kind((samples_count,)),
            kind((pairs,)),
        ],
        compiler_params=pltpu.CompilerParams(
            collective_id=0, has_side_effects=True, vmem_limit_bytes=56 * 2**20
        ),
        name="whiten",
    )(comp_sizes, labels.reshape(tiles, LANES), observed).astype(BF16)


def pairs_fit(rows, width, slots, samples_count, groups_count):
    return (
        slots == samples_count
        and samples_count % 4 == 0
        and groups_count > 1
        and rows * samples_count < CMAX
        and (2 * width // slots) % LANES == 0
        and rows % 16 == 0
    )


def body(observed, labels, comp_sizes):
    rows, width = observed.shape
    slots = comp_sizes.shape[0]
    samples_count = lax.axis_size("samples")
    groups_count = lax.axis_size("groups")
    if pairs_fit(rows, width, slots, samples_count, groups_count):
        return paired(observed, labels, comp_sizes, samples_count, groups_count)
    slot_here = slots // samples_count
    tiles = width // LANES
    samples = rows * samples_count
    kind = pltpu.SemaphoreType.DMA
    table = pltpu.VMEM((tiles, slots, LANES), jnp.int32)
    wide_tiles = pltpu.VMEM((tiles, rows, LANES), F32)
    blocks = pltpu.VMEM((samples_count, slot_here, rows, CMAX), BF16)
    work = [pltpu.VMEM((CMAX, CMAX), F32)] * 2 if samples >= CMAX else []
    return pl.pallas_call(
        functools.partial(
            fused_kernel, samples_count, groups_count, float(samples * width * groups_count)
        ),
        out_shape=pltpu.VMEM((rows, width), F32),
        in_specs=[pl.BlockSpec(memory_space=pltpu.HBM)] * 3,
        out_specs=VMEM,
        scratch_shapes=[
            pltpu.SMEM(comp_sizes.shape, jnp.int32),
            pltpu.VMEM((tiles, LANES), jnp.int32),
            pltpu.VMEM((rows, width), BF16),
            kind((3,)),
            wide_tiles,
            table,
            table,
            pltpu.VMEM((tiles, LANES), jnp.int32),
            wide_tiles,
            blocks,
            blocks,
            blocks,
            blocks,
            pltpu.VMEM((8, LANES), F32),
            pltpu.VMEM((groups_count - 1, 8, LANES), F32),
            pltpu.VMEM((8, LANES), F32),
            pltpu.VMEM((samples_count - 1, 8, LANES), F32),
            *work,
            kind((groups_count - 1,)),
            kind((groups_count - 1,)),
            kind((samples_count - 1,)),
            kind((samples_count - 1,)),
            kind((samples_count - 1,)),
            kind((samples_count - 1,)),
            kind((samples_count - 1,)),
            kind((samples_count,)),
        ],
        compiler_params=pltpu.CompilerParams(
            collective_id=0, has_side_effects=True, vmem_limit_bytes=56 * 2**20
        ),
        name="whiten",
    )(comp_sizes, labels.reshape(tiles, LANES), observed).astype(BF16)


def solution(mesh):
    return jax.shard_map(
        body,
        mesh=mesh,
        in_specs=(P("samples", "groups"), P("groups"), P("groups")),
        out_specs=P("samples", "groups"),
        check_vma=False,
    )
```

```python
import functools

import jax
import jax.numpy as jnp
from jax import lax
from jax.experimental import pallas as pl
from jax.experimental.pallas import tpu as pltpu
from jax.sharding import PartitionSpec as P

CMAX = 512
ITERS = 5
LANES = 128
UNROLL_LIMIT = 1024

shrink = 0.2
ridge = 0.5

BF16 = jnp.bfloat16
F32 = jnp.float32
HIGHEST = lax.Precision.HIGHEST
MESH = pl.DeviceIdType.MESH
VMEM = pl.BlockSpec(memory_space=pltpu.VMEM)


def loop(count, step, carry, unrolled):
    if unrolled:
        for i in range(count):
            carry = step(i, carry)
        return carry
    return lax.fori_loop(0, count, step, carry)


def lane_gather(values, index):
    return jnp.take_along_axis(values, index, axis=1)


def thirds(value):
    high = value.astype(BF16)
    rest = value - high.astype(F32)
    middle = rest.astype(BF16)
    low = (rest - middle.astype(F32)).astype(BF16)
    return high, middle, low


def products(lefts, right):
    extent = right.shape[0]
    high, middle, low = thirds(right)
    left_high, left_middle, left_low = thirds(jnp.concatenate(lefts, axis=0))
    pair = jnp.concatenate([high, middle], axis=1)
    main = jnp.dot(
        jnp.concatenate([left_high, left_middle], axis=1),
        jnp.concatenate([pair, pair], axis=0),
        preferred_element_type=F32,
    )
    small = jnp.dot(
        jnp.concatenate([left_high, left_low], axis=1),
        jnp.concatenate([low, high], axis=0),
        preferred_element_type=F32,
    )
    whole = (small + main[:, extent:]) + main[:, :extent]
    return [whole[i * extent : (i + 1) * extent] for i in range(len(lefts))]


def eye(extent, value):
    down = lax.broadcasted_iota(jnp.int32, (extent, extent), 0)
    across = lax.broadcasted_iota(jnp.int32, (extent, extent), 1)
    return jnp.where(down == across, jnp.broadcast_to(value, (extent, extent)), 0.0)


def scale_and_bound(samples, gram_peak, squares, size, average):
    target = squares / samples / size
    lift = shrink * target + ridge * average
    weight = (1.0 - shrink) / samples
    return weight, lift, weight * gram_peak + lift


def whiten_rows(block, turned, inner, squares, peak, size, average, out):
    samples = block.shape[0]
    weight, lift, bound = scale_and_bound(samples, peak, squares, size, average)
    inverse_bound = 1.0 / bound
    v = inner * (weight * inverse_bound)
    e = 1.0 - lift * inverse_bound
    c = jnp.ones_like(e)
    u = d = None
    for step in range(ITERS):
        lefts = [] if step == ITERS - 1 else [v] if step == 0 else [v, u]
        results = products(lefts + ([d] if step > 1 else []), v)
        if step == 0:
            d, u = eye(samples, -c), eye(samples, 2.0 * e) - v
        else:
            through = results[-1] if step > 1 else -v
            d = (1.0 + e) * d - c * u - through
            if lefts:
                u = 2.0 * e * u - results[1]
        if lefts:
            v = 2.0 * e * v - results[0]
        c = c * (1.0 + e)
        e = e * e
    mixed = sum(jnp.dot(piece, block, preferred_element_type=F32) for piece in reversed(thirds(d)))
    mixed = mixed * (weight * inverse_bound)
    width = block.shape[1]
    stacked = jnp.concatenate(thirds(mixed), axis=0)
    wide_turned = jnp.concatenate([turned] * 3, axis=1)
    inverse = jnp.dot(wide_turned, stacked, preferred_element_type=F32) * inverse_bound
    inverse = (inverse + eye(width, c * inverse_bound)).astype(BF16)
    out(jnp.dot(block, inverse, preferred_element_type=F32).astype(BF16))


def whiten_columns(block, gram_ref, current_ref, squares, peak, size, average, out):
    samples, width = block.shape
    weight, lift, bound = scale_and_bound(samples, peak, squares, size, average)
    gram_ref[...] = weight * gram_ref[...] + eye(width, lift)
    current_ref[...] = eye(width, 1.0 / bound)

    def sweep(i, carry):
        current = current_ref[...]
        product = jnp.dot(gram_ref[...], current, precision=HIGHEST, preferred_element_type=F32)
        current_ref[...] = jnp.dot(
            current, eye(width, jnp.full((1, 1), 2.0, F32)) - product, precision=HIGHEST, preferred_element_type=F32
        )
        return carry

    lax.fori_loop(0, ITERS, sweep, 0)
    out(jnp.dot(block, current_ref[...].astype(BF16), preferred_element_type=F32).astype(BF16))


def fused_kernel(
    samples_count,
    groups_count,
    entries,
    size_hbm,
    label_hbm,
    observed_hbm,
    result_ref,
    size_ref,
    label_ref,
    observed_ref,
    load_sem,
    sorted_ref,
    high_ref,
    turn_ref,
    place_ref,
    filled_ref,
    packed_ref,
    held_ref,
    done_ref,
    back_ref,
    energy_ref,
    group_ref,
    total_ref,
    all_ref,
    *rest,
):
    *work, group_send, group_recv, total_send, total_recv, out_send, out_recv, back_send, back_recv = rest
    me = lax.axis_index("samples")
    group = lax.axis_index("groups")
    _, slot_here, rows, width = packed_ref.shape
    samples = samples_count * rows
    slots = samples_count * slot_here
    tiles = sorted_ref.shape[0]
    parts = width // LANES
    unrolled = tiles * slots <= UNROLL_LIMIT
    order = sorted(range(1, samples_count), key=lambda k: abs(2 * k - samples_count))

    def ahead(k):
        return lax.rem(me + k, samples_count)

    def behind(k):
        return lax.rem(me + samples_count - k, samples_count)

    def copy(source, target, send, recv, sample, other):
        return pltpu.make_async_remote_copy(
            src_ref=source,
            dst_ref=target,
            send_sem=send,
            recv_sem=recv,
            device_id=(sample, other),
            device_id_type=MESH,
        )

    def columns(t):
        return pl.ds(t * LANES if isinstance(t, int) else pl.multiple_of(t * LANES, LANES), LANES)

    loads = [
        pltpu.make_async_copy(source, target, load_sem.at[i])
        for i, (source, target) in enumerate(
            ((label_hbm, label_ref), (observed_hbm, observed_ref), (size_hbm, size_ref))
        )
    ]
    for item in loads:
        item.start()
    barrier = pltpu.get_barrier_semaphore()
    for k in range(1, samples_count):
        pl.semaphore_signal(barrier, inc=1, device_id=(ahead(k), group), device_id_type=MESH)
    for k in range(1, groups_count):
        other = lax.rem(group + k, groups_count)
        pl.semaphore_signal(barrier, inc=1, device_id=(me, other), device_id_type=MESH)

    for item in loads:
        item.wait()

    first = group * slots
    slot = lax.broadcasted_iota(jnp.int32, (slots, LANES), 0)
    down = lax.broadcasted_iota(jnp.int32, (LANES, LANES), 0)
    across = lax.broadcasted_iota(jnp.int32, (LANES, LANES), 1)
    upto = (down <= across).astype(BF16)
    ones = jnp.ones((LANES, LANES), BF16)

    def compare(t):
        label = label_ref[pl.ds(t, 1), :] - first
        return (label == slot).astype(F32), (label < slot).astype(F32)

    def counts(equal, less):
        rank = jnp.dot(equal.astype(BF16), upto, preferred_element_type=F32) - 1.0
        count = jnp.dot(equal.astype(BF16), ones, preferred_element_type=F32)
        before = jnp.dot(less.astype(BF16), ones, preferred_element_type=F32)
        return rank, count, before

    if unrolled:
        pairs = [compare(t) for t in range(tiles)]
        stacked = counts(*(jnp.concatenate(items, axis=0) for items in zip(*pairs)))

    def sort_tile(t, carry):
        base, energy = carry
        if unrolled:
            equal = pairs[t][0]
            rank, count, before = (item[t * slots : (t + 1) * slots] for item in stacked)
        else:
            equal, less = compare(t)
            rank, count, before = counts(equal, less)
        local = jnp.sum(equal * (before + rank), axis=0, keepdims=True).astype(jnp.int32)
        whole = slot.astype(F32) * CMAX + base + rank
        place_ref[pl.ds(t, 1), :] = jnp.sum(equal * whole, axis=0, keepdims=True).astype(jnp.int32)
        block = observed_ref[:, columns(t)]
        choose = (down == local).astype(BF16)
        sorted_ref[t] = lax.dot_general(
            block, choose, (((1,), (1,)), ((), ())), preferred_element_type=F32
        )
        high_ref[t] = (base + count).astype(jnp.int32)
        turn_ref[t] = (before - base).astype(jnp.int32)
        wide = block.astype(F32)
        square = wide * wide
        for r in range(0, rows, 8):
            energy = energy + square[r : r + 8]
        return base + count, energy

    start = (jnp.zeros((slots, LANES), F32), jnp.zeros((8, LANES), F32))
    _, total = loop(tiles, sort_tile, start, unrolled)
    energy_ref[...] = total

    lane = lax.broadcasted_iota(jnp.int32, (rows, LANES), 1)

    def pack_slot(sample, h, target):
        c = sample * slot_here + h

        def add_tile(i, packed):
            t = tiles - 1 - i
            high = jnp.broadcast_to(high_ref[t, pl.ds(c, 1), :], (rows, LANES))
            turn = jnp.broadcast_to(turn_ref[t, pl.ds(c, 1), :], (rows, LANES))
            moved = lane_gather(sorted_ref[t], (lane + turn) & (LANES - 1))
            return tuple(
                jnp.where(lane + q * LANES < high, moved, packed[q])
                for q in range(parts)
            )

        zero = jnp.zeros((rows, LANES), F32)
        packed = loop(tiles, add_tile, (zero,) * parts, unrolled)
        for q in range(parts):
            target[:, q * LANES : (q + 1) * LANES] = packed[q].astype(BF16)

    group_copies = [
        copy(
            energy_ref,
            group_ref.at[k - 1],
            group_send.at[k - 1],
            group_recv.at[k - 1],
            me,
            lax.rem(group + k, groups_count),
        )
        for k in range(1, groups_count)
    ]
    out_copies = {
        k: copy(packed_ref.at[k], held_ref.at[k], out_send.at[k - 1], out_recv.at[k - 1], ahead(k), group)
        for k in order
    }
    total_copies = [
        copy(total_ref, all_ref.at[k - 1], total_send.at[k - 1], total_recv.at[k - 1], ahead(k), group)
        for k in order
    ]
    back_copies = [
        copy(done_ref.at[k], back_ref.at[me], back_send.at[k - 1], back_recv.at[me], behind(k), group)
        for k in order
    ]

    for k in order:
        for h in range(slot_here):
            pack_slot(ahead(k), h, packed_ref.at[k, h])
    pl.semaphore_wait(barrier, samples_count + groups_count - 2)
    for item in group_copies:
        item.start()
    for k in order:
        out_copies[k].start()
    for h in range(slot_here):
        pack_slot(me, h, held_ref.at[0, h])
    for item in group_copies:
        item.wait_recv()
    for k in range(groups_count - 1):
        total = total + group_ref[k]
    total_ref[...] = total
    for item in total_copies:
        item.start()
    for k in order:
        out_copies[k].wait_recv()

    average = None
    for h in range(slot_here):
        block = held_ref[:, h].reshape(samples, width)
        turned = block.T
        wide = block.astype(F32)
        squares = jnp.sum(jnp.sum(wide * wide, axis=0, keepdims=True), axis=1, keepdims=True)
        sums = jnp.zeros((1, width), F32)
        for r in range(0, width, LANES):
            part = jnp.dot(turned[r : r + LANES], block, preferred_element_type=F32)
            if work:
                work[0][r : r + LANES, :] = part
            sums = sums + jnp.sum(jnp.abs(part), axis=0, keepdims=True)
        peak = jnp.max(sums, axis=1, keepdims=True)
        if not work:
            inner = lax.dot_general(block, block, (((1,), (1,)), ((), ())), preferred_element_type=F32)
        if average is None:
            for item in total_copies:
                item.wait_recv()
            for k in range(samples_count - 1):
                total = total + all_ref[k]
            energy = jnp.sum(jnp.sum(total, axis=0, keepdims=True), axis=1, keepdims=True)
            average = energy / entries
        size = jnp.full((1, 1), size_ref[me * slot_here + h], jnp.int32).astype(F32)

        def out(value):
            done_ref[:, h] = value.reshape(samples_count, rows, width)

        if work:
            whiten_columns(block, work[0], work[1], squares, peak, size, average, out)
        else:
            whiten_rows(block, turned, inner, squares, peak, size, average, out)

    for item in back_copies:
        item.start()

    def fill(sample, source, opening):
        for h in range(slot_here):
            wide = [source[h, :, q * LANES : (q + 1) * LANES].astype(F32) for q in range(parts)]

            def fill_tile(t, carry):
                place = jnp.broadcast_to(place_ref[pl.ds(t, 1), :], (rows, LANES))
                index = place & (LANES - 1)
                tile = (place >> (LANES.bit_length() - 1)) - (sample * slot_here + h) * parts
                if opening and h == 0:
                    value = jnp.zeros((rows, LANES), F32)
                else:
                    value = filled_ref[t]
                for q in range(parts):
                    value = jnp.where(tile == q, lane_gather(wide[q], index), value)
                filled_ref[t] = value
                return carry

            loop(tiles, fill_tile, 0, unrolled)

    fill(me, done_ref.at[0], True)
    for k in reversed(order):
        copy(
            done_ref.at[k], back_ref.at[ahead(k)], back_send.at[k - 1], back_recv.at[ahead(k)], ahead(k), group
        ).wait_recv()
        fill(ahead(k), back_ref.at[ahead(k)], False)

    def finish(t, carry):
        result_ref[:, columns(t)] = filled_ref[t]
        return carry

    loop(tiles, finish, 0, unrolled)
    for item in group_copies + list(out_copies.values()) + total_copies + back_copies:
        item.wait_send()


def pieces(value):
    high = value.astype(BF16)
    return high, (value - high.astype(F32)).astype(BF16)


def stack_product(lefts, right):
    extent = right[0].shape[1]
    pair = jnp.concatenate(right, axis=1)
    left = jnp.concatenate([jnp.concatenate(item, axis=1) for item in lefts], axis=0)
    both = jnp.dot(left, jnp.concatenate([pair, pair], axis=0), preferred_element_type=F32)
    whole = both[:, extent:] + both[:, :extent]
    rows = right[0].shape[0]
    return [whole[i * rows : (i + 1) * rows] for i in range(len(lefts))]


def residual_series(gram, peak, box):
    extent = gram.shape[0]
    one = eye(extent, jnp.ones((1, 1), F32))
    positive = peak > 0.0
    unit = jnp.where(positive, 1.0 / jnp.where(positive, peak, 1.0), 0.0)
    first = one - gram * unit
    cut = pieces(first)
    (second,) = stack_product([cut], cut)
    cut_second = pieces(second)
    yield
    third, power = stack_product([cut, cut_second], cut_second)
    yield
    e = box[0]
    square = e * e
    count = 1.0 + e
    series = one * (count + square) + first * (e + square) + second * square
    total = (one + first) + (second + third)
    count = count * (1.0 + square)
    before, raised = e * square, square * square
    yield
    for _ in range(2):
        cut = pieces(power)
        power, through, more = stack_product([cut, pieces(series), pieces(total)], cut)
        series = series + through * raised + total * (before * count)
        total = total + more
        count = count * (1.0 + raised)
        before, raised = before * raised, raised * raised
        yield
    (through,) = stack_product([pieces(series)], pieces(power))
    yield series + through * raised + total * (before * count), count * (1.0 + raised)


def residual_powers(gram, peak):
    extent = gram.shape[0]
    one = eye(extent, jnp.ones((1, 1), F32))
    positive = peak > 0.0
    unit = jnp.where(positive, 1.0 / jnp.where(positive, peak, 1.0), 0.0)
    power = {1: one - gram * unit}
    cut = {1: pieces(power[1])}
    yield

    def extend(names, by):
        for name, value in zip(names, stack_product([cut[n - by] for n in names], cut[by])):
            power[name] = value
            cut[name] = pieces(value)

    extend([2], 1)
    yield
    extend([3, 4], 2)
    yield
    extend([5, 6, 7, 8], 4)
    total = {8: one + sum(power[i] for i in range(1, 8))}
    first = pieces(total[8])
    yield
    power[16], more = stack_product([cut[8], first], cut[8])
    total[16] = total[8] + more
    cut[16] = pieces(power[16])
    yield
    power[24], more = stack_product([cut[8], first], cut[16])
    total[24] = total[16] + more
    yield power, total


def powers_series(power, total, e):
    raised = {0: jnp.ones_like(e), 1: e}
    for i in (2, 3, 4, 5, 6, 7, 8):
        raised[i] = raised[i // 2] * raised[i - i // 2]
    raised[15] = raised[8] * raised[7]
    raised[16] = raised[8] * raised[8]
    raised[23] = raised[16] * raised[7]
    raised[24] = raised[16] * raised[8]
    tail = {7: raised[7]}
    for i in range(6, -1, -1):
        tail[i] = raised[i] + tail[i + 1]
    eight = tail[0]
    extent = power[1].shape[0]
    series = eye(extent, eight - raised[7])
    for i in range(1, 7):
        series = series + power[i] * (tail[i] - raised[7])
    spread = sum(power[i] * raised[i] for i in (8, 16, 24))
    rest = sum(total[i] * (eight * raised[i - 1]) for i in (8, 16, 24))
    (through,) = stack_product([pieces(spread)], pieces(series))
    whole = eight * (1.0 + raised[8]) * (1.0 + raised[16])
    return through + (series + rest), whole


def late_series(gram, peak, box):
    maker = residual_powers(gram, peak)
    for _ in range(5):
        next(maker)
        yield
    power, total = next(maker)
    yield
    yield powers_series(power, total, box[0])


def whiten_pair(leads, block, odd, sizes, flag_ref, same_ref, inverse_ref, share_total, wait_average, out):
    samples, width = block.shape
    turned = block.T
    second = block * odd.astype(BF16)
    first = block - second
    both = jnp.concatenate([first, second], axis=0)
    second_turned = turned * flag_ref[...]
    both_turned = jnp.concatenate([turned - second_turned, second_turned], axis=1)
    inner = jnp.dot(block, both_turned, preferred_element_type=F32)
    lines = [jnp.zeros((1, LANES), F32)] * (width // LANES)
    for r in range(0, width, LANES):
        part = jnp.abs(jnp.dot(both_turned[r : r + LANES], both[:, r:], preferred_element_type=F32))
        down = jnp.sum(part, axis=0, keepdims=True)
        for q in range(r, width, LANES):
            lines[q // LANES] = lines[q // LANES] + down[:, q - r : q - r + LANES]
        if r + LANES < width:
            right = sum(part[:, q - r : q - r + LANES] for q in range(r + LANES, width, LANES))
            lines[r // LANES] = lines[r // LANES] + jnp.sum(right.T, axis=0, keepdims=True)
    sums = jnp.concatenate(lines, axis=1)
    peaks = [jnp.max(sums * side, axis=1, keepdims=True) for side in (1.0 - odd, odd)]
    grams = [inner[:, :samples], inner[:, samples:]]
    traces = []
    for gram in grams:
        kept = gram * eye(samples, jnp.ones((1, 1), F32))
        traces.append(jnp.sum(jnp.sum(kept, axis=0, keepdims=True), axis=1, keepdims=True))
    boxes = [[], []]
    make = residual_series if leads else late_series
    makers = [make(gram, peak, box) for gram, peak, box in zip(grams, peaks, boxes)]
    for step in range(2 if leads else 6):
        for maker in makers:
            next(maker)
        if leads and step == 0:
            share_total()
    average = wait_average()
    weight = (1.0 - shrink) / samples
    inverse_bounds = []
    for peak, trace, size, box in zip(peaks, traces, sizes, boxes):
        lift = shrink * (trace / samples / size) + ridge * average
        inverse_bound = 1.0 / (weight * peak + lift)
        box.append(weight * peak * inverse_bound)
        inverse_bounds.append(inverse_bound)
    for _ in range(4 if leads else 1):
        found = [next(maker) for maker in makers]
    middles = [piece for middle, _ in found for piece in pieces(middle)]
    wholes = [whole for _, whole in found]
    factors = [weight * inverse_bound for inverse_bound in inverse_bounds]

    def by_side(values):
        return jnp.where(odd > 0.5, values[1], values[0])

    mixed = jnp.dot(
        jnp.concatenate(middles, axis=1),
        jnp.concatenate([first, first, second, second], axis=0),
        preferred_element_type=F32,
    )
    mixed = mixed * (-by_side(factors))
    stacked = jnp.concatenate(pieces(mixed), axis=0)
    scale = by_side(inverse_bounds)
    peak_line = by_side(wholes)
    wide_turned = jnp.concatenate([turned, turned], axis=1)
    for r in range(0, width, LANES):
        part = jnp.dot(wide_turned[r : r + LANES], stacked[:, r:], preferred_element_type=F32)
        line = eye(LANES, jnp.ones((1, 1), F32)) * peak_line[:, r : r + LANES]
        for q in range(r, width, LANES):
            value = part[:, q - r : q - r + LANES]
            if q == r:
                value = value + line
            value = (value * scale[:, q : q + LANES]).astype(BF16)
            value = value * same_ref[r : r + LANES, q : q + LANES]
            inverse_ref[r : r + LANES, q : q + LANES] = value
            if q > r:
                inverse_ref[q : q + LANES, r : r + LANES] = value.T
    out(jnp.dot(block, inverse_ref[...], preferred_element_type=F32).astype(BF16))


def pair_kernel(
    samples_count,
    groups_count,
    entries,
    size_hbm,
    label_hbm,
    observed_hbm,
    result_ref,
    size_ref,
    label_ref,
    observed_ref,
    load_sem,
    sorted_ref,
    side_ref,
    high_ref,
    turn_ref,
    place_ref,
    packed_ref,
    held_ref,
    odd_ref,
    flag_ref,
    same_ref,
    inverse_ref,
    done_ref,
    back_ref,
    energy_ref,
    all_ref,
    total_ref,
    total_in_ref,
    energy_send,
    energy_recv,
    total_send,
    total_recv,
    out_send,
    out_recv,
    back_send,
    back_recv,
):
    me = lax.axis_index("samples")
    group = lax.axis_index("groups")
    pairs, rows, width = packed_ref.shape
    tiles = sorted_ref.shape[0]
    table_rows = high_ref.shape[1]
    parts = width // LANES
    opening = samples_count // 4
    mine = jnp.clip(me - opening, 0, pairs - 1)
    inverts = (me >= opening) & (me < opening + pairs)
    hub_group = group == 0
    later = jnp.minimum(group, 1)
    number = group * samples_count + me
    devices = samples_count * groups_count

    def copy(source, target, send, recv, sample, other):
        return pltpu.make_async_remote_copy(
            src_ref=source,
            dst_ref=target,
            send_sem=send,
            recv_sem=recv,
            device_id=(sample, other),
            device_id_type=MESH,
        )

    def signal(sample, other):
        pl.semaphore_signal(barrier, inc=1, device_id=(sample, other), device_id_type=MESH)

    loads = [
        pltpu.make_async_copy(source, target, load_sem.at[i])
        for i, (source, target) in enumerate(
            ((label_hbm, label_ref), (observed_hbm, observed_ref), (size_hbm, size_ref))
        )
    ]
    for item in loads:
        item.start()
    barrier = pltpu.get_barrier_semaphore()

    @pl.when(inverts)
    def _():
        for k in range(1, samples_count):
            signal(lax.rem(me + k, samples_count), group)

    @pl.when(inverts & hub_group)
    def _():
        for j in range(1, groups_count):
            for k in range(samples_count):
                signal(lax.rem(me + k, samples_count), lax.rem(group + j, groups_count))

    for item in loads:
        item.wait()

    slots = 2 * pairs
    first = group * slots
    slot = lax.broadcasted_iota(jnp.int32, (table_rows, LANES), 0)
    down = lax.broadcasted_iota(jnp.int32, (LANES, LANES), 0)
    across = lax.broadcasted_iota(jnp.int32, (LANES, LANES), 1)
    upto = (down <= across).astype(BF16)
    ones = jnp.ones((LANES, LANES), BF16)
    energy = jnp.zeros((8, LANES), F32)
    equals, lesses, blocks, sides = [], [], [], []
    for t in range(tiles):
        block = observed_ref[:, t * LANES : (t + 1) * LANES]
        wide = block.astype(F32)
        square = wide * wide
        for r in range(0, rows, 8):
            energy = energy + square[r : r + 8]
        label = label_ref[pl.ds(t, 1), :] - first
        pair = label >> 1
        equals.append((pair == slot).astype(F32))
        lesses.append((pair < slot).astype(F32))
        side = jnp.broadcast_to((label & 1).astype(F32), (rows, LANES)).astype(BF16)
        blocks.append(jnp.concatenate([block, side], axis=0))
    energy_ref[0] = jnp.sum(energy, axis=0, keepdims=True)
    all_ref[number] = energy_ref[0]
    equal_all = jnp.concatenate(equals, axis=0).astype(BF16)
    less_all = jnp.concatenate(lesses, axis=0).astype(BF16)
    ranks = jnp.dot(equal_all, upto, preferred_element_type=F32) - 1.0
    counts = jnp.dot(equal_all, ones, preferred_element_type=F32)
    befores = jnp.dot(less_all, ones, preferred_element_type=F32)
    base = jnp.zeros((table_rows, LANES), F32)
    for t in range(tiles):
        span = slice(t * table_rows, (t + 1) * table_rows)
        rank, count, before, equal = ranks[span], counts[span], befores[span], equals[t]
        local = jnp.sum(equal * (before + rank), axis=0, keepdims=True).astype(jnp.int32)
        whole = slot.astype(F32) * width + base + rank
        place_ref[pl.ds(t, 1), :] = jnp.sum(equal * whole, axis=0, keepdims=True).astype(jnp.int32)
        choose = (down == local).astype(BF16)
        ordered = lax.dot_general(blocks[t], choose, (((1,), (1,)), ((), ())), preferred_element_type=F32)
        sorted_ref[t] = ordered[:rows]
        side_ref[t] = ordered[rows : rows + 8]
        high_ref[t] = (base + count).astype(jnp.int32)
        turn_ref[t] = (before - base).astype(jnp.int32)
        base = base + count

    lane = lax.broadcasted_iota(jnp.int32, (rows, LANES), 1)

    def reach(t):
        return range(max(0, parts - tiles + t), min(parts, t + 1))

    def pack(c, source, height):
        packed = [jnp.zeros((height, LANES), F32)] * parts
        place = lane[:height]
        for t in reversed(range(tiles)):
            high = jnp.broadcast_to(high_ref[t, pl.ds(c, 1), :], (height, LANES))
            turn = jnp.broadcast_to(turn_ref[t, pl.ds(c, 1), :], (height, LANES))
            moved = lane_gather(source[t], (place + turn) & (LANES - 1))
            for q in reach(t):
                packed[q] = jnp.where(place + q * LANES < high, moved, packed[q])
        return packed

    for p in range(pairs):
        for q, value in enumerate(pack(p, sorted_ref, rows)):
            packed_ref[p, :, q * LANES : (q + 1) * LANES] = value.astype(BF16)

    near_half = me < opening + pairs // 2
    far_first = [jnp.where(near_half, pairs - 1 - k, k) for k in range(pairs)]
    out_copies = [
        copy(packed_ref.at[p], held_ref.at[me], out_send.at[k], out_recv.at[me], opening + p, group)
        for k, p in enumerate(far_first)
    ]
    hubs = [(opening + p, 0) for p in range(pairs)]
    energy_copies = [
        copy(energy_ref.at[0], all_ref.at[number], energy_send.at[i], energy_recv, sample, other)
        for i, (sample, other) in enumerate(hubs)
    ]

    def elsewhere(sample, other=None):
        away = me != sample
        return away if other is None else away | (group != other)

    pl.semaphore_wait(barrier, (1 + later) * pairs - inverts.astype(jnp.int32))
    for item, hub in zip(energy_copies, hubs):
        pl.when(elsewhere(*hub))(item.start)
    for p, item in zip(far_first, out_copies):
        pl.when(elsewhere(opening + p))(item.start)

    total_copies = [
        copy(total_ref, total_in_ref, total_send.at[g - 1], total_recv, me, g) for g in range(1, groups_count)
    ]

    @pl.when(inverts)
    def _():
        held_ref[me] = packed_ref[mine]
        odd = jnp.concatenate(pack(mine, side_ref, 8), axis=1)
        odd_ref[...] = odd
        odd_turned = jnp.concatenate([odd] * (LANES // 8), axis=0).T
        flag_ref[...] = odd_turned.astype(BF16)
        for r in range(0, width, LANES):
            for q in range(0, width, LANES):
                same = odd_turned[r : r + LANES] == jnp.broadcast_to(odd[:1, q : q + LANES], (LANES, LANES))
                same_ref[r : r + LANES, q : q + LANES] = same.astype(F32).astype(BF16)
        for k in range(1, samples_count):
            other = lax.rem(me + k, samples_count)
            copy(
                packed_ref.at[0], held_ref.at[other], out_send.at[0], out_recv.at[other], me, group
            ).wait_recv()

        def share_total():
            rest = all_ref.at[pl.ds(0, devices - 1)]
            copy(rest, rest, energy_send.at[0], energy_recv, me, group).wait_recv()
            total = jnp.sum(all_ref[...], axis=0)
            total_in_ref[...] = total
            total_ref[...] = total
            for item in total_copies:
                item.start()

        def wait_average(leads):
            if not leads:
                total_copies[0].wait_recv()
            return jnp.sum(total_in_ref[...], axis=1, keepdims=True) / entries

        def out(value):
            done_ref[...] = value.reshape(samples_count, rows, width)

        sizes = [
            jnp.full((1, 1), size_ref[2 * mine + h], jnp.int32).astype(F32) for h in range(2)
        ]
        def invert(leads):
            block = held_ref[...].reshape(samples_count * rows, width)
            whiten_pair(
                leads,
                block,
                odd_ref[:1],
                sizes,
                flag_ref,
                same_ref,
                inverse_ref,
                share_total,
                functools.partial(wait_average, leads),
                out,
            )

        pl.when(hub_group)(functools.partial(invert, True))
        pl.when(group != 0)(functools.partial(invert, False))
        for k in range(1, samples_count):
            other = lax.rem(me + k, samples_count)
            copy(
                done_ref.at[other], back_ref.at[mine], back_send.at[k - 1], back_recv.at[mine], other, group
            ).start()
        back_ref[mine] = done_ref[me]

    for k in range(pairs):
        p = jnp.where(me < opening + pairs // 2, k, pairs - 1 - k)

        @pl.when(elsewhere(opening + p))
        def _():
            copy(
                done_ref.at[0], back_ref.at[p], back_send.at[0], back_recv.at[p], opening + p, group
            ).wait_recv()

        wide = [back_ref[p, :, q * LANES : (q + 1) * LANES].astype(F32) for q in range(parts)]
        for t in range(tiles):
            place = jnp.broadcast_to(place_ref[pl.ds(t, 1), :], (rows, LANES))
            index = place & (LANES - 1)
            tile = (place >> (LANES.bit_length() - 1)) - p * parts
            if k == 0:
                value = jnp.zeros((rows, LANES), F32)
            else:
                value = result_ref[:, t * LANES : (t + 1) * LANES]
            for q in reach(t):
                value = jnp.where(tile == q, lane_gather(wide[q], index), value)
            result_ref[:, t * LANES : (t + 1) * LANES] = value

    for item, hub in zip(energy_copies, hubs):
        pl.when(elsewhere(*hub))(item.wait_send)
    for p, item in zip(far_first, out_copies):
        pl.when(elsewhere(opening + p))(item.wait_send)

    @pl.when(inverts & hub_group)
    def _():
        for item in total_copies:
            item.wait_send()


    @pl.when(inverts)
    def _():
        for k in range(1, samples_count):
            other = lax.rem(me + k, samples_count)
            copy(
                done_ref.at[other], back_ref.at[mine], back_send.at[k - 1], back_recv.at[mine], other, group
            ).wait_send()


def paired(observed, labels, comp_sizes, samples_count, groups_count):
    rows, width = observed.shape
    pairs = comp_sizes.shape[0] // 2
    pair_width = width // pairs
    tiles = width // LANES
    devices = samples_count * groups_count
    table_rows = -(-pairs // 8) * 8
    kind = pltpu.SemaphoreType.DMA
    table = pltpu.VMEM((tiles, table_rows, LANES), jnp.int32)
    square = pltpu.VMEM((pair_width, pair_width), BF16)
    blocks = pltpu.VMEM((samples_count, rows, pair_width), BF16)
    kept = pltpu.VMEM((pairs, rows, pair_width), BF16)
    line = pltpu.VMEM((1, LANES), F32)
    return pl.pallas_call(
        functools.partial(
            pair_kernel, samples_count, groups_count, float(samples_count * rows * width * groups_count)
        ),
        out_shape=pltpu.VMEM((rows, width), F32),
        in_specs=[pl.BlockSpec(memory_space=pltpu.HBM)] * 3,
        out_specs=VMEM,
        scratch_shapes=[
            pltpu.SMEM(comp_sizes.shape, jnp.int32),
            pltpu.VMEM((tiles, LANES), jnp.int32),
            pltpu.VMEM((rows, width), BF16),
            kind((3,)),
            pltpu.VMEM((tiles, rows, LANES), F32),
            pltpu.VMEM((tiles, 8, LANES), F32),
            table,
            table,
            pltpu.VMEM((tiles, LANES), jnp.int32),
            kept,
            blocks,
            pltpu.VMEM((8, pair_width), F32),
            pltpu.VMEM((pair_width, LANES), BF16),
            square,
            square,
            blocks,
            kept,
            pltpu.VMEM((1, 1, LANES), F32),
            pltpu.VMEM((devices, 1, LANES), F32),
            line,
            line,
            kind((pairs,)),
            kind,
            kind((groups_count - 1,)),
            kind,
            kind((pairs,)),
            kind((samples_count,)),
            kind((samples_count,)),
            kind((pairs,)),
        ],
        compiler_params=pltpu.CompilerParams(
            collective_id=0, has_side_effects=True, vmem_limit_bytes=56 * 2**20
        ),
        name="whiten",
    )(comp_sizes, labels.reshape(tiles, LANES), observed).astype(BF16)


def pairs_fit(rows, width, slots, samples_count, groups_count):
    return (
        slots == samples_count
        and samples_count % 4 == 0
        and groups_count > 1
        and rows * samples_count < CMAX
        and (2 * width // slots) % LANES == 0
        and rows % 16 == 0
    )


def body(observed, labels, comp_sizes):
    rows, width = observed.shape
    slots = comp_sizes.shape[0]
    samples_count = lax.axis_size("samples")
    groups_count = lax.axis_size("groups")
    if pairs_fit(rows, width, slots, samples_count, groups_count):
        return paired(observed, labels, comp_sizes, samples_count, groups_count)
    slot_here = slots // samples_count
    tiles = width // LANES
    samples = rows * samples_count
    kind = pltpu.SemaphoreType.DMA
    table = pltpu.VMEM((tiles, slots, LANES), jnp.int32)
    wide_tiles = pltpu.VMEM((tiles, rows, LANES), F32)
    blocks = pltpu.VMEM((samples_count, slot_here, rows, CMAX), BF16)
    work = [pltpu.VMEM((CMAX, CMAX), F32)] * 2 if samples >= CMAX else []
    return pl.pallas_call(
        functools.partial(
            fused_kernel, samples_count, groups_count, float(samples * width * groups_count)
        ),
        out_shape=pltpu.VMEM((rows, width), F32),
        in_specs=[pl.BlockSpec(memory_space=pltpu.HBM)] * 3,
        out_specs=VMEM,
        scratch_shapes=[
            pltpu.SMEM(comp_sizes.shape, jnp.int32),
            pltpu.VMEM((tiles, LANES), jnp.int32),
            pltpu.VMEM((rows, width), BF16),
            kind((3,)),
            wide_tiles,
            table,
            table,
            pltpu.VMEM((tiles, LANES), jnp.int32),
            wide_tiles,
            blocks,
            blocks,
            blocks,
            blocks,
            pltpu.VMEM((8, LANES), F32),
            pltpu.VMEM((groups_count - 1, 8, LANES), F32),
            pltpu.VMEM((8, LANES), F32),
            pltpu.VMEM((samples_count - 1, 8, LANES), F32),
            *work,
            kind((groups_count - 1,)),
            kind((groups_count - 1,)),
            kind((samples_count - 1,)),
            kind((samples_count - 1,)),
            kind((samples_count - 1,)),
            kind((samples_count - 1,)),
            kind((samples_count - 1,)),
            kind((samples_count,)),
        ],
        compiler_params=pltpu.CompilerParams(
            collective_id=0, has_side_effects=True, vmem_limit_bytes=56 * 2**20
        ),
        name="whiten",
    )(comp_sizes, labels.reshape(tiles, LANES), observed).astype(BF16)


def solution(mesh):
    return jax.shard_map(
        body,
        mesh=mesh,
        in_specs=(P("samples", "groups"), P("groups"), P("groups")),
        out_specs=P("samples", "groups"),
        check_vma=False,
    )
```

```python
import functools

import jax
import jax.numpy as jnp
from jax import lax
from jax.experimental import pallas as pl
from jax.experimental.pallas import tpu as pltpu
from jax.sharding import PartitionSpec as P

CMAX = 512
ITERS = 5
LANES = 128
UNROLL_LIMIT = 1024

shrink = 0.2
ridge = 0.5

BF16 = jnp.bfloat16
F32 = jnp.float32
HIGHEST = lax.Precision.HIGHEST
MESH = pl.DeviceIdType.MESH
VMEM = pl.BlockSpec(memory_space=pltpu.VMEM)


def loop(count, step, carry, unrolled):
    if unrolled:
        for i in range(count):
            carry = step(i, carry)
        return carry
    return lax.fori_loop(0, count, step, carry)


def lane_gather(values, index):
    return jnp.take_along_axis(values, index, axis=1)


def thirds(value):
    high = value.astype(BF16)
    rest = value - high.astype(F32)
    middle = rest.astype(BF16)
    low = (rest - middle.astype(F32)).astype(BF16)
    return high, middle, low


def products(lefts, right):
    extent = right.shape[0]
    high, middle, low = thirds(right)
    left_high, left_middle, left_low = thirds(jnp.concatenate(lefts, axis=0))
    pair = jnp.concatenate([high, middle], axis=1)
    main = jnp.dot(
        jnp.concatenate([left_high, left_middle], axis=1),
        jnp.concatenate([pair, pair], axis=0),
        preferred_element_type=F32,
    )
    small = jnp.dot(
        jnp.concatenate([left_high, left_low], axis=1),
        jnp.concatenate([low, high], axis=0),
        preferred_element_type=F32,
    )
    whole = (small + main[:, extent:]) + main[:, :extent]
    return [whole[i * extent : (i + 1) * extent] for i in range(len(lefts))]


def eye(extent, value):
    down = lax.broadcasted_iota(jnp.int32, (extent, extent), 0)
    across = lax.broadcasted_iota(jnp.int32, (extent, extent), 1)
    return jnp.where(down == across, jnp.broadcast_to(value, (extent, extent)), 0.0)


def scale_and_bound(samples, gram_peak, squares, size, average):
    target = squares / samples / size
    lift = shrink * target + ridge * average
    weight = (1.0 - shrink) / samples
    return weight, lift, weight * gram_peak + lift


def whiten_rows(block, turned, inner, squares, peak, size, average, out):
    samples = block.shape[0]
    weight, lift, bound = scale_and_bound(samples, peak, squares, size, average)
    inverse_bound = 1.0 / bound
    v = inner * (weight * inverse_bound)
    e = 1.0 - lift * inverse_bound
    c = jnp.ones_like(e)
    u = d = None
    for step in range(ITERS):
        lefts = [] if step == ITERS - 1 else [v] if step == 0 else [v, u]
        results = products(lefts + ([d] if step > 1 else []), v)
        if step == 0:
            d, u = eye(samples, -c), eye(samples, 2.0 * e) - v
        else:
            through = results[-1] if step > 1 else -v
            d = (1.0 + e) * d - c * u - through
            if lefts:
                u = 2.0 * e * u - results[1]
        if lefts:
            v = 2.0 * e * v - results[0]
        c = c * (1.0 + e)
        e = e * e
    mixed = sum(jnp.dot(piece, block, preferred_element_type=F32) for piece in reversed(thirds(d)))
    mixed = mixed * (weight * inverse_bound)
    width = block.shape[1]
    stacked = jnp.concatenate(thirds(mixed), axis=0)
    wide_turned = jnp.concatenate([turned] * 3, axis=1)
    inverse = jnp.dot(wide_turned, stacked, preferred_element_type=F32) * inverse_bound
    inverse = (inverse + eye(width, c * inverse_bound)).astype(BF16)
    out(jnp.dot(block, inverse, preferred_element_type=F32).astype(BF16))


def whiten_columns(block, gram_ref, current_ref, squares, peak, size, average, out):
    samples, width = block.shape
    weight, lift, bound = scale_and_bound(samples, peak, squares, size, average)
    gram_ref[...] = weight * gram_ref[...] + eye(width, lift)
    current_ref[...] = eye(width, 1.0 / bound)

    def sweep(i, carry):
        current = current_ref[...]
        product = jnp.dot(gram_ref[...], current, precision=HIGHEST, preferred_element_type=F32)
        current_ref[...] = jnp.dot(
            current, eye(width, jnp.full((1, 1), 2.0, F32)) - product, precision=HIGHEST, preferred_element_type=F32
        )
        return carry

    lax.fori_loop(0, ITERS, sweep, 0)
    out(jnp.dot(block, current_ref[...].astype(BF16), preferred_element_type=F32).astype(BF16))


def fused_kernel(
    samples_count,
    groups_count,
    entries,
    size_hbm,
    label_hbm,
    observed_hbm,
    result_ref,
    size_ref,
    label_ref,
    observed_ref,
    load_sem,
    sorted_ref,
    high_ref,
    turn_ref,
    place_ref,
    filled_ref,
    packed_ref,
    held_ref,
    done_ref,
    back_ref,
    energy_ref,
    group_ref,
    total_ref,
    all_ref,
    *rest,
):
    *work, group_send, group_recv, total_send, total_recv, out_send, out_recv, back_send, back_recv = rest
    me = lax.axis_index("samples")
    group = lax.axis_index("groups")
    _, slot_here, rows, width = packed_ref.shape
    samples = samples_count * rows
    slots = samples_count * slot_here
    tiles = sorted_ref.shape[0]
    parts = width // LANES
    unrolled = tiles * slots <= UNROLL_LIMIT
    order = sorted(range(1, samples_count), key=lambda k: abs(2 * k - samples_count))

    def ahead(k):
        return lax.rem(me + k, samples_count)

    def behind(k):
        return lax.rem(me + samples_count - k, samples_count)

    def copy(source, target, send, recv, sample, other):
        return pltpu.make_async_remote_copy(
            src_ref=source,
            dst_ref=target,
            send_sem=send,
            recv_sem=recv,
            device_id=(sample, other),
            device_id_type=MESH,
        )

    def columns(t):
        return pl.ds(t * LANES if isinstance(t, int) else pl.multiple_of(t * LANES, LANES), LANES)

    loads = [
        pltpu.make_async_copy(source, target, load_sem.at[i])
        for i, (source, target) in enumerate(
            ((label_hbm, label_ref), (observed_hbm, observed_ref), (size_hbm, size_ref))
        )
    ]
    for item in loads:
        item.start()
    barrier = pltpu.get_barrier_semaphore()
    for k in range(1, samples_count):
        pl.semaphore_signal(barrier, inc=1, device_id=(ahead(k), group), device_id_type=MESH)
    for k in range(1, groups_count):
        other = lax.rem(group + k, groups_count)
        pl.semaphore_signal(barrier, inc=1, device_id=(me, other), device_id_type=MESH)

    for item in loads:
        item.wait()

    first = group * slots
    slot = lax.broadcasted_iota(jnp.int32, (slots, LANES), 0)
    down = lax.broadcasted_iota(jnp.int32, (LANES, LANES), 0)
    across = lax.broadcasted_iota(jnp.int32, (LANES, LANES), 1)
    upto = (down <= across).astype(BF16)
    ones = jnp.ones((LANES, LANES), BF16)

    def compare(t):
        label = label_ref[pl.ds(t, 1), :] - first
        return (label == slot).astype(F32), (label < slot).astype(F32)

    def counts(equal, less):
        rank = jnp.dot(equal.astype(BF16), upto, preferred_element_type=F32) - 1.0
        count = jnp.dot(equal.astype(BF16), ones, preferred_element_type=F32)
        before = jnp.dot(less.astype(BF16), ones, preferred_element_type=F32)
        return rank, count, before

    if unrolled:
        pairs = [compare(t) for t in range(tiles)]
        stacked = counts(*(jnp.concatenate(items, axis=0) for items in zip(*pairs)))

    def sort_tile(t, carry):
        base, energy = carry
        if unrolled:
            equal = pairs[t][0]
            rank, count, before = (item[t * slots : (t + 1) * slots] for item in stacked)
        else:
            equal, less = compare(t)
            rank, count, before = counts(equal, less)
        local = jnp.sum(equal * (before + rank), axis=0, keepdims=True).astype(jnp.int32)
        whole = slot.astype(F32) * CMAX + base + rank
        place_ref[pl.ds(t, 1), :] = jnp.sum(equal * whole, axis=0, keepdims=True).astype(jnp.int32)
        block = observed_ref[:, columns(t)]
        choose = (down == local).astype(BF16)
        sorted_ref[t] = lax.dot_general(
            block, choose, (((1,), (1,)), ((), ())), preferred_element_type=F32
        )
        high_ref[t] = (base + count).astype(jnp.int32)
        turn_ref[t] = (before - base).astype(jnp.int32)
        wide = block.astype(F32)
        square = wide * wide
        for r in range(0, rows, 8):
            energy = energy + square[r : r + 8]
        return base + count, energy

    start = (jnp.zeros((slots, LANES), F32), jnp.zeros((8, LANES), F32))
    _, total = loop(tiles, sort_tile, start, unrolled)
    energy_ref[...] = total

    lane = lax.broadcasted_iota(jnp.int32, (rows, LANES), 1)

    def pack_slot(sample, h, target):
        c = sample * slot_here + h

        def add_tile(i, packed):
            t = tiles - 1 - i
            high = jnp.broadcast_to(high_ref[t, pl.ds(c, 1), :], (rows, LANES))
            turn = jnp.broadcast_to(turn_ref[t, pl.ds(c, 1), :], (rows, LANES))
            moved = lane_gather(sorted_ref[t], (lane + turn) & (LANES - 1))
            return tuple(
                jnp.where(lane + q * LANES < high, moved, packed[q])
                for q in range(parts)
            )

        zero = jnp.zeros((rows, LANES), F32)
        packed = loop(tiles, add_tile, (zero,) * parts, unrolled)
        for q in range(parts):
            target[:, q * LANES : (q + 1) * LANES] = packed[q].astype(BF16)

    group_copies = [
        copy(
            energy_ref,
            group_ref.at[k - 1],
            group_send.at[k - 1],
            group_recv.at[k - 1],
            me,
            lax.rem(group + k, groups_count),
        )
        for k in range(1, groups_count)
    ]
    out_copies = {
        k: copy(packed_ref.at[k], held_ref.at[k], out_send.at[k - 1], out_recv.at[k - 1], ahead(k), group)
        for k in order
    }
    total_copies = [
        copy(total_ref, all_ref.at[k - 1], total_send.at[k - 1], total_recv.at[k - 1], ahead(k), group)
        for k in order
    ]
    back_copies = [
        copy(done_ref.at[k], back_ref.at[me], back_send.at[k - 1], back_recv.at[me], behind(k), group)
        for k in order
    ]

    for k in order:
        for h in range(slot_here):
            pack_slot(ahead(k), h, packed_ref.at[k, h])
    pl.semaphore_wait(barrier, samples_count + groups_count - 2)
    for item in group_copies:
        item.start()
    for k in order:
        out_copies[k].start()
    for h in range(slot_here):
        pack_slot(me, h, held_ref.at[0, h])
    for item in group_copies:
        item.wait_recv()
    for k in range(groups_count - 1):
        total = total + group_ref[k]
    total_ref[...] = total
    for item in total_copies:
        item.start()
    for k in order:
        out_copies[k].wait_recv()

    average = None
    for h in range(slot_here):
        block = held_ref[:, h].reshape(samples, width)
        turned = block.T
        wide = block.astype(F32)
        squares = jnp.sum(jnp.sum(wide * wide, axis=0, keepdims=True), axis=1, keepdims=True)
        sums = jnp.zeros((1, width), F32)
        for r in range(0, width, LANES):
            part = jnp.dot(turned[r : r + LANES], block, preferred_element_type=F32)
            if work:
                work[0][r : r + LANES, :] = part
            sums = sums + jnp.sum(jnp.abs(part), axis=0, keepdims=True)
        peak = jnp.max(sums, axis=1, keepdims=True)
        if not work:
            inner = lax.dot_general(block, block, (((1,), (1,)), ((), ())), preferred_element_type=F32)
        if average is None:
            for item in total_copies:
                item.wait_recv()
            for k in range(samples_count - 1):
                total = total + all_ref[k]
            energy = jnp.sum(jnp.sum(total, axis=0, keepdims=True), axis=1, keepdims=True)
            average = energy / entries
        size = jnp.full((1, 1), size_ref[me * slot_here + h], jnp.int32).astype(F32)

        def out(value):
            done_ref[:, h] = value.reshape(samples_count, rows, width)

        if work:
            whiten_columns(block, work[0], work[1], squares, peak, size, average, out)
        else:
            whiten_rows(block, turned, inner, squares, peak, size, average, out)

    for item in back_copies:
        item.start()

    def fill(sample, source, opening):
        for h in range(slot_here):
            wide = [source[h, :, q * LANES : (q + 1) * LANES].astype(F32) for q in range(parts)]

            def fill_tile(t, carry):
                place = jnp.broadcast_to(place_ref[pl.ds(t, 1), :], (rows, LANES))
                index = place & (LANES - 1)
                tile = (place >> (LANES.bit_length() - 1)) - (sample * slot_here + h) * parts
                if opening and h == 0:
                    value = jnp.zeros((rows, LANES), F32)
                else:
                    value = filled_ref[t]
                for q in range(parts):
                    value = jnp.where(tile == q, lane_gather(wide[q], index), value)
                filled_ref[t] = value
                return carry

            loop(tiles, fill_tile, 0, unrolled)

    fill(me, done_ref.at[0], True)
    for k in reversed(order):
        copy(
            done_ref.at[k], back_ref.at[ahead(k)], back_send.at[k - 1], back_recv.at[ahead(k)], ahead(k), group
        ).wait_recv()
        fill(ahead(k), back_ref.at[ahead(k)], False)

    def finish(t, carry):
        result_ref[:, columns(t)] = filled_ref[t]
        return carry

    loop(tiles, finish, 0, unrolled)
    for item in group_copies + list(out_copies.values()) + total_copies + back_copies:
        item.wait_send()


def pieces(value):
    high = value.astype(BF16)
    return high, (value - high.astype(F32)).astype(BF16)


def stack_product(lefts, right):
    extent = right[0].shape[1]
    pair = jnp.concatenate(right, axis=1)
    left = jnp.concatenate([jnp.concatenate(item, axis=1) for item in lefts], axis=0)
    both = jnp.dot(left, jnp.concatenate([pair, pair], axis=0), preferred_element_type=F32)
    whole = both[:, extent:] + both[:, :extent]
    rows = right[0].shape[0]
    return [whole[i * rows : (i + 1) * rows] for i in range(len(lefts))]


def residual_series(gram, peak, box):
    extent = gram.shape[0]
    one = eye(extent, jnp.ones((1, 1), F32))
    positive = peak > 0.0
    unit = jnp.where(positive, 1.0 / jnp.where(positive, peak, 1.0), 0.0)
    first = one - gram * unit
    cut = pieces(first)
    (second,) = stack_product([cut], cut)
    cut_second = pieces(second)
    yield
    third, power = stack_product([cut, cut_second], cut_second)
    yield
    e = box[0]
    square = e * e
    count = 1.0 + e
    series = one * (count + square) + first * (e + square) + second * square
    total = (one + first) + (second + third)
    count = count * (1.0 + square)
    before, raised = e * square, square * square
    yield
    for _ in range(2):
        cut = pieces(power)
        power, through, more = stack_product([cut, pieces(series), pieces(total)], cut)
        series = series + through * raised + total * (before * count)
        total = total + more
        count = count * (1.0 + raised)
        before, raised = before * raised, raised * raised
        yield
    (through,) = stack_product([pieces(series)], pieces(power))
    yield series + through * raised + total * (before * count), count * (1.0 + raised)


def residual_powers(gram, peak):
    extent = gram.shape[0]
    one = eye(extent, jnp.ones((1, 1), F32))
    positive = peak > 0.0
    unit = jnp.where(positive, 1.0 / jnp.where(positive, peak, 1.0), 0.0)
    power = {1: one - gram * unit}
    cut = {1: pieces(power[1])}
    yield

    def extend(names, by):
        for name, value in zip(names, stack_product([cut[n - by] for n in names], cut[by])):
            power[name] = value
            cut[name] = pieces(value)

    extend([2], 1)
    yield
    extend([3, 4], 2)
    yield
    extend([5, 6, 7, 8], 4)
    total = {8: one + sum(power[i] for i in range(1, 8))}
    first = pieces(total[8])
    yield
    power[16], more = stack_product([cut[8], first], cut[8])
    total[16] = total[8] + more
    cut[16] = pieces(power[16])
    yield
    power[24], more = stack_product([cut[8], first], cut[16])
    total[24] = total[16] + more
    yield power, total


def powers_series(power, total, e):
    raised = {0: jnp.ones_like(e), 1: e}
    for i in (2, 3, 4, 5, 6, 7, 8):
        raised[i] = raised[i // 2] * raised[i - i // 2]
    raised[15] = raised[8] * raised[7]
    raised[16] = raised[8] * raised[8]
    raised[23] = raised[16] * raised[7]
    raised[24] = raised[16] * raised[8]
    tail = {7: raised[7]}
    for i in range(6, -1, -1):
        tail[i] = raised[i] + tail[i + 1]
    eight = tail[0]
    extent = power[1].shape[0]
    series = eye(extent, eight - raised[7])
    for i in range(1, 7):
        series = series + power[i] * (tail[i] - raised[7])
    spread = sum(power[i] * raised[i] for i in (8, 16, 24))
    rest = sum(total[i] * (eight * raised[i - 1]) for i in (8, 16, 24))
    (through,) = stack_product([pieces(spread)], pieces(series))
    whole = eight * (1.0 + raised[8]) * (1.0 + raised[16])
    return through + (series + rest), whole


def late_series(gram, peak, box):
    maker = residual_powers(gram, peak)
    for _ in range(5):
        next(maker)
        yield
    power, total = next(maker)
    yield
    yield powers_series(power, total, box[0])


def whiten_pair(leads, block, odd, sizes, flag_ref, same_ref, inverse_ref, share_total, wait_average, out):
    samples, width = block.shape
    turned = block.T
    second = block * odd.astype(BF16)
    first = block - second
    both = jnp.concatenate([first, second], axis=0)
    second_turned = turned * flag_ref[...]
    both_turned = jnp.concatenate([turned - second_turned, second_turned], axis=1)
    inner = jnp.dot(block, both_turned, preferred_element_type=F32)
    lines = [jnp.zeros((1, LANES), F32)] * (width // LANES)
    for r in range(0, width, LANES):
        part = jnp.abs(jnp.dot(both_turned[r : r + LANES], both[:, r:], preferred_element_type=F32))
        down = jnp.sum(part, axis=0, keepdims=True)
        for q in range(r, width, LANES):
            lines[q // LANES] = lines[q // LANES] + down[:, q - r : q - r + LANES]
        if r + LANES < width:
            right = sum(part[:, q - r : q - r + LANES] for q in range(r + LANES, width, LANES))
            lines[r // LANES] = lines[r // LANES] + jnp.sum(right.T, axis=0, keepdims=True)
    sums = jnp.concatenate(lines, axis=1)
    peaks = [jnp.max(sums * side, axis=1, keepdims=True) for side in (1.0 - odd, odd)]
    grams = [inner[:, :samples], inner[:, samples:]]
    traces = []
    for gram in grams:
        kept = gram * eye(samples, jnp.ones((1, 1), F32))
        traces.append(jnp.sum(jnp.sum(kept, axis=0, keepdims=True), axis=1, keepdims=True))
    boxes = [[], []]
    make = residual_series if leads else late_series
    makers = [make(gram, peak, box) for gram, peak, box in zip(grams, peaks, boxes)]
    for step in range(2 if leads else 6):
        for maker in makers:
            next(maker)
        if leads and step == 0:
            share_total()
    average = wait_average()
    weight = (1.0 - shrink) / samples
    inverse_bounds = []
    for peak, trace, size, box in zip(peaks, traces, sizes, boxes):
        lift = shrink * (trace / samples / size) + ridge * average
        inverse_bound = 1.0 / (weight * peak + lift)
        box.append(weight * peak * inverse_bound)
        inverse_bounds.append(inverse_bound)
    for _ in range(4 if leads else 1):
        found = [next(maker) for maker in makers]
    middles = [piece for middle, _ in found for piece in pieces(middle)]
    wholes = [whole for _, whole in found]
    factors = [weight * inverse_bound for inverse_bound in inverse_bounds]

    def by_side(values):
        return jnp.where(odd > 0.5, values[1], values[0])

    mixed = jnp.dot(
        jnp.concatenate(middles, axis=1),
        jnp.concatenate([first, first, second, second], axis=0),
        preferred_element_type=F32,
    )
    mixed = mixed * (-by_side(factors))
    stacked = jnp.concatenate(pieces(mixed), axis=0)
    scale = by_side(inverse_bounds)
    peak_line = by_side(wholes)
    wide_turned = jnp.concatenate([turned, turned], axis=1)
    for r in range(0, width, LANES):
        part = jnp.dot(wide_turned[r : r + LANES], stacked[:, r:], preferred_element_type=F32)
        line = eye(LANES, jnp.ones((1, 1), F32)) * peak_line[:, r : r + LANES]
        for q in range(r, width, LANES):
            value = part[:, q - r : q - r + LANES]
            if q == r:
                value = value + line
            value = (value * scale[:, q : q + LANES]).astype(BF16)
            value = value * same_ref[r : r + LANES, q : q + LANES]
            inverse_ref[r : r + LANES, q : q + LANES] = value
            if q > r:
                inverse_ref[q : q + LANES, r : r + LANES] = value.T
    out(jnp.dot(block, inverse_ref[...], preferred_element_type=F32).astype(BF16))


def pair_kernel(
    samples_count,
    groups_count,
    entries,
    size_hbm,
    label_hbm,
    observed_hbm,
    result_ref,
    size_ref,
    label_ref,
    observed_ref,
    load_sem,
    sorted_ref,
    side_ref,
    high_ref,
    turn_ref,
    place_ref,
    packed_ref,
    held_ref,
    odd_ref,
    flag_ref,
    same_ref,
    inverse_ref,
    done_ref,
    back_ref,
    energy_ref,
    all_ref,
    total_ref,
    total_in_ref,
    energy_send,
    energy_recv,
    total_send,
    total_recv,
    out_send,
    out_recv,
    back_send,
    back_recv,
):
    me = lax.axis_index("samples")
    group = lax.axis_index("groups")
    pairs, rows, width = packed_ref.shape
    tiles = sorted_ref.shape[0]
    table_rows = high_ref.shape[1]
    parts = width // LANES
    opening = samples_count // 4
    mine = jnp.clip(me - opening, 0, pairs - 1)
    inverts = (me >= opening) & (me < opening + pairs)
    hub_group = group == 0
    later = jnp.minimum(group, 1)
    number = group * samples_count + me
    devices = samples_count * groups_count

    def copy(source, target, send, recv, sample, other):
        return pltpu.make_async_remote_copy(
            src_ref=source,
            dst_ref=target,
            send_sem=send,
            recv_sem=recv,
            device_id=(sample, other),
            device_id_type=MESH,
        )

    def signal(sample, other):
        pl.semaphore_signal(barrier, inc=1, device_id=(sample, other), device_id_type=MESH)

    loads = [
        pltpu.make_async_copy(source, target, load_sem.at[i])
        for i, (source, target) in enumerate(
            ((label_hbm, label_ref), (observed_hbm, observed_ref), (size_hbm, size_ref))
        )
    ]
    for item in loads:
        item.start()
    barrier = pltpu.get_barrier_semaphore()

    @pl.when(inverts)
    def _():
        for k in range(1, samples_count):
            signal(lax.rem(me + k, samples_count), group)

    @pl.when(inverts & hub_group)
    def _():
        for j in range(1, groups_count):
            for k in range(samples_count):
                signal(lax.rem(me + k, samples_count), lax.rem(group + j, groups_count))

    for item in loads:
        item.wait()

    slots = 2 * pairs
    first = group * slots
    slot = lax.broadcasted_iota(jnp.int32, (table_rows, LANES), 0)
    down = lax.broadcasted_iota(jnp.int32, (LANES, LANES), 0)
    across = lax.broadcasted_iota(jnp.int32, (LANES, LANES), 1)
    upto = (down <= across).astype(BF16)
    ones = jnp.ones((LANES, LANES), BF16)
    energy = jnp.zeros((8, LANES), F32)
    equals, lesses, blocks, sides = [], [], [], []
    for t in range(tiles):
        block = observed_ref[:, t * LANES : (t + 1) * LANES]
        wide = block.astype(F32)
        square = wide * wide
        for r in range(0, rows, 8):
            energy = energy + square[r : r + 8]
        label = label_ref[pl.ds(t, 1), :] - first
        pair = label >> 1
        equals.append((pair == slot).astype(F32))
        lesses.append((pair < slot).astype(F32))
        side = jnp.broadcast_to((label & 1).astype(F32), (rows, LANES)).astype(BF16)
        blocks.append(jnp.concatenate([block, side], axis=0))
    energy_ref[0] = jnp.sum(energy, axis=0, keepdims=True)
    all_ref[number] = energy_ref[0]
    equal_all = jnp.concatenate(equals, axis=0).astype(BF16)
    less_all = jnp.concatenate(lesses, axis=0).astype(BF16)
    ranks = jnp.dot(equal_all, upto, preferred_element_type=F32) - 1.0
    counts = jnp.dot(equal_all, ones, preferred_element_type=F32)
    befores = jnp.dot(less_all, ones, preferred_element_type=F32)
    base = jnp.zeros((table_rows, LANES), F32)
    for t in range(tiles):
        span = slice(t * table_rows, (t + 1) * table_rows)
        rank, count, before, equal = ranks[span], counts[span], befores[span], equals[t]
        local = jnp.sum(equal * (before + rank), axis=0, keepdims=True).astype(jnp.int32)
        whole = slot.astype(F32) * width + base + rank
        place_ref[pl.ds(t, 1), :] = jnp.sum(equal * whole, axis=0, keepdims=True).astype(jnp.int32)
        choose = (down == local).astype(BF16)
        ordered = lax.dot_general(blocks[t], choose, (((1,), (1,)), ((), ())), preferred_element_type=F32)
        sorted_ref[t] = ordered[:rows]
        side_ref[t] = ordered[rows : rows + 8]
        high_ref[t] = (base + count).astype(jnp.int32)
        turn_ref[t] = (before - base).astype(jnp.int32)
        base = base + count

    lane = lax.broadcasted_iota(jnp.int32, (rows, LANES), 1)

    def reach(t):
        return range(max(0, parts - tiles + t), min(parts, t + 1))

    def pack(c, source, height):
        packed = [jnp.zeros((height, LANES), F32)] * parts
        place = lane[:height]
        for t in reversed(range(tiles)):
            high = jnp.broadcast_to(high_ref[t, pl.ds(c, 1), :], (height, LANES))
            turn = jnp.broadcast_to(turn_ref[t, pl.ds(c, 1), :], (height, LANES))
            moved = lane_gather(source[t], (place + turn) & (LANES - 1))
            for q in reach(t):
                packed[q] = jnp.where(place + q * LANES < high, moved, packed[q])
        return packed

    for p in range(pairs):
        for q, value in enumerate(pack(p, sorted_ref, rows)):
            packed_ref[p, :, q * LANES : (q + 1) * LANES] = value.astype(BF16)

    near_half = me < opening + pairs // 2
    far_first = [jnp.where(near_half, pairs - 1 - k, k) for k in range(pairs)]
    out_copies = [
        copy(packed_ref.at[p], held_ref.at[me], out_send.at[k], out_recv.at[me], opening + p, group)
        for k, p in enumerate(far_first)
    ]
    hubs = [(opening + p, 0) for p in range(pairs)]
    energy_copies = [
        copy(energy_ref.at[0], all_ref.at[number], energy_send.at[i], energy_recv, sample, other)
        for i, (sample, other) in enumerate(hubs)
    ]

    def elsewhere(sample, other=None):
        away = me != sample
        return away if other is None else away | (group != other)

    pl.semaphore_wait(barrier, (1 + later) * pairs - inverts.astype(jnp.int32))
    for item, hub in zip(energy_copies, hubs):
        pl.when(elsewhere(*hub))(item.start)
    for p, item in zip(far_first, out_copies):
        pl.when(elsewhere(opening + p))(item.start)

    total_copies = [
        copy(total_ref, total_in_ref, total_send.at[g - 1], total_recv, me, g) for g in range(1, groups_count)
    ]

    @pl.when(inverts)
    def _():
        held_ref[me] = packed_ref[mine]
        odd = jnp.concatenate(pack(mine, side_ref, 8), axis=1)
        odd_ref[...] = odd
        odd_turned = jnp.concatenate([odd] * (LANES // 8), axis=0).T
        flag_ref[...] = odd_turned.astype(BF16)
        for r in range(0, width, LANES):
            for q in range(0, width, LANES):
                same = odd_turned[r : r + LANES] == jnp.broadcast_to(odd[:1, q : q + LANES], (LANES, LANES))
                same_ref[r : r + LANES, q : q + LANES] = same.astype(F32).astype(BF16)
        for k in range(1, samples_count):
            other = lax.rem(me + k, samples_count)
            copy(
                packed_ref.at[0], held_ref.at[other], out_send.at[0], out_recv.at[other], me, group
            ).wait_recv()

        def share_total():
            rest = all_ref.at[pl.ds(0, devices - 1)]
            copy(rest, rest, energy_send.at[0], energy_recv, me, group).wait_recv()
            total = jnp.sum(all_ref[...], axis=0)
            total_in_ref[...] = total
            total_ref[...] = total
            for item in total_copies:
                item.start()

        def wait_average(leads):
            if not leads:
                total_copies[0].wait_recv()
            return jnp.sum(total_in_ref[...], axis=1, keepdims=True) / entries

        def out(value):
            done_ref[...] = value.reshape(samples_count, rows, width)

        sizes = [
            jnp.full((1, 1), size_ref[2 * mine + h], jnp.int32).astype(F32) for h in range(2)
        ]
        def invert(leads):
            block = held_ref[...].reshape(samples_count * rows, width)
            whiten_pair(
                leads,
                block,
                odd_ref[:1],
                sizes,
                flag_ref,
                same_ref,
                inverse_ref,
                share_total,
                functools.partial(wait_average, leads),
                out,
            )

        pl.when(hub_group)(functools.partial(invert, True))
        pl.when(group != 0)(functools.partial(invert, False))
        for k in range(samples_count - 1):
            other = k + (me <= k).astype(jnp.int32)
            copy(
                done_ref.at[other], back_ref.at[mine], back_send.at[k], back_recv.at[mine], other, group
            ).start()
        back_ref[mine] = done_ref[me]

    for k in range(pairs):
        p = jnp.where(me < opening + pairs // 2, k, pairs - 1 - k)

        @pl.when(elsewhere(opening + p))
        def _():
            copy(
                done_ref.at[0], back_ref.at[p], back_send.at[0], back_recv.at[p], opening + p, group
            ).wait_recv()

        wide = [back_ref[p, :, q * LANES : (q + 1) * LANES].astype(F32) for q in range(parts)]
        for t in range(tiles):
            place = jnp.broadcast_to(place_ref[pl.ds(t, 1), :], (rows, LANES))
            index = place & (LANES - 1)
            tile = (place >> (LANES.bit_length() - 1)) - p * parts
            if k == 0:
                value = jnp.zeros((rows, LANES), F32)
            else:
                value = result_ref[:, t * LANES : (t + 1) * LANES]
            for q in reach(t):
                value = jnp.where(tile == q, lane_gather(wide[q], index), value)
            result_ref[:, t * LANES : (t + 1) * LANES] = value

    for item, hub in zip(energy_copies, hubs):
        pl.when(elsewhere(*hub))(item.wait_send)
    for p, item in zip(far_first, out_copies):
        pl.when(elsewhere(opening + p))(item.wait_send)

    @pl.when(inverts & hub_group)
    def _():
        for item in total_copies:
            item.wait_send()


    @pl.when(inverts)
    def _():
        for k in range(samples_count - 1):
            other = k + (me <= k).astype(jnp.int32)
            copy(
                done_ref.at[other], back_ref.at[mine], back_send.at[k], back_recv.at[mine], other, group
            ).wait_send()


def paired(observed, labels, comp_sizes, samples_count, groups_count):
    rows, width = observed.shape
    pairs = comp_sizes.shape[0] // 2
    pair_width = width // pairs
    tiles = width // LANES
    devices = samples_count * groups_count
    table_rows = -(-pairs // 8) * 8
    kind = pltpu.SemaphoreType.DMA
    table = pltpu.VMEM((tiles, table_rows, LANES), jnp.int32)
    square = pltpu.VMEM((pair_width, pair_width), BF16)
    blocks = pltpu.VMEM((samples_count, rows, pair_width), BF16)
    kept = pltpu.VMEM((pairs, rows, pair_width), BF16)
    line = pltpu.VMEM((1, LANES), F32)
    return pl.pallas_call(
        functools.partial(
            pair_kernel, samples_count, groups_count, float(samples_count * rows * width * groups_count)
        ),
        out_shape=pltpu.VMEM((rows, width), F32),
        in_specs=[pl.BlockSpec(memory_space=pltpu.HBM)] * 3,
        out_specs=VMEM,
        scratch_shapes=[
            pltpu.SMEM(comp_sizes.shape, jnp.int32),
            pltpu.VMEM((tiles, LANES), jnp.int32),
            pltpu.VMEM((rows, width), BF16),
            kind((3,)),
            pltpu.VMEM((tiles, rows, LANES), F32),
            pltpu.VMEM((tiles, 8, LANES), F32),
            table,
            table,
            pltpu.VMEM((tiles, LANES), jnp.int32),
            kept,
            blocks,
            pltpu.VMEM((8, pair_width), F32),
            pltpu.VMEM((pair_width, LANES), BF16),
            square,
            square,
            blocks,
            kept,
            pltpu.VMEM((1, 1, LANES), F32),
            pltpu.VMEM((devices, 1, LANES), F32),
            line,
            line,
            kind((pairs,)),
            kind,
            kind((groups_count - 1,)),
            kind,
            kind((pairs,)),
            kind((samples_count,)),
            kind((samples_count,)),
            kind((pairs,)),
        ],
        compiler_params=pltpu.CompilerParams(
            collective_id=0, has_side_effects=True, vmem_limit_bytes=56 * 2**20
        ),
        name="whiten",
    )(comp_sizes, labels.reshape(tiles, LANES), observed).astype(BF16)


def pairs_fit(rows, width, slots, samples_count, groups_count):
    return (
        slots == samples_count
        and samples_count % 4 == 0
        and groups_count > 1
        and rows * samples_count < CMAX
        and (2 * width // slots) % LANES == 0
        and rows % 16 == 0
    )


def body(observed, labels, comp_sizes):
    rows, width = observed.shape
    slots = comp_sizes.shape[0]
    samples_count = lax.axis_size("samples")
    groups_count = lax.axis_size("groups")
    if pairs_fit(rows, width, slots, samples_count, groups_count):
        return paired(observed, labels, comp_sizes, samples_count, groups_count)
    slot_here = slots // samples_count
    tiles = width // LANES
    samples = rows * samples_count
    kind = pltpu.SemaphoreType.DMA
    table = pltpu.VMEM((tiles, slots, LANES), jnp.int32)
    wide_tiles = pltpu.VMEM((tiles, rows, LANES), F32)
    blocks = pltpu.VMEM((samples_count, slot_here, rows, CMAX), BF16)
    work = [pltpu.VMEM((CMAX, CMAX), F32)] * 2 if samples >= CMAX else []
    return pl.pallas_call(
        functools.partial(
            fused_kernel, samples_count, groups_count, float(samples * width * groups_count)
        ),
        out_shape=pltpu.VMEM((rows, width), F32),
        in_specs=[pl.BlockSpec(memory_space=pltpu.HBM)] * 3,
        out_specs=VMEM,
        scratch_shapes=[
            pltpu.SMEM(comp_sizes.shape, jnp.int32),
            pltpu.VMEM((tiles, LANES), jnp.int32),
            pltpu.VMEM((rows, width), BF16),
            kind((3,)),
            wide_tiles,
            table,
            table,
            pltpu.VMEM((tiles, LANES), jnp.int32),
            wide_tiles,
            blocks,
            blocks,
            blocks,
            blocks,
            pltpu.VMEM((8, LANES), F32),
            pltpu.VMEM((groups_count - 1, 8, LANES), F32),
            pltpu.VMEM((8, LANES), F32),
            pltpu.VMEM((samples_count - 1, 8, LANES), F32),
            *work,
            kind((groups_count - 1,)),
            kind((groups_count - 1,)),
            kind((samples_count - 1,)),
            kind((samples_count - 1,)),
            kind((samples_count - 1,)),
            kind((samples_count - 1,)),
            kind((samples_count - 1,)),
            kind((samples_count,)),
        ],
        compiler_params=pltpu.CompilerParams(
            collective_id=0, has_side_effects=True, vmem_limit_bytes=56 * 2**20
        ),
        name="whiten",
    )(comp_sizes, labels.reshape(tiles, LANES), observed).astype(BF16)


def solution(mesh):
    return jax.shard_map(
        body,
        mesh=mesh,
        in_specs=(P("samples", "groups"), P("groups"), P("groups")),
        out_specs=P("samples", "groups"),
        check_vma=False,
    )
```

```python
import functools

import jax
import jax.numpy as jnp
from jax import lax
from jax.experimental import pallas as pl
from jax.experimental.pallas import tpu as pltpu
from jax.sharding import PartitionSpec as P

CMAX = 512
ITERS = 5
LANES = 128
UNROLL_LIMIT = 1024

shrink = 0.2
ridge = 0.5

BF16 = jnp.bfloat16
F32 = jnp.float32
HIGHEST = lax.Precision.HIGHEST
MESH = pl.DeviceIdType.MESH
VMEM = pl.BlockSpec(memory_space=pltpu.VMEM)


def loop(count, step, carry, unrolled):
    if unrolled:
        for i in range(count):
            carry = step(i, carry)
        return carry
    return lax.fori_loop(0, count, step, carry)


def lane_gather(values, index):
    return jnp.take_along_axis(values, index, axis=1)


def thirds(value):
    high = value.astype(BF16)
    rest = value - high.astype(F32)
    middle = rest.astype(BF16)
    low = (rest - middle.astype(F32)).astype(BF16)
    return high, middle, low


def products(lefts, right):
    extent = right.shape[0]
    high, middle, low = thirds(right)
    left_high, left_middle, left_low = thirds(jnp.concatenate(lefts, axis=0))
    pair = jnp.concatenate([high, middle], axis=1)
    main = jnp.dot(
        jnp.concatenate([left_high, left_middle], axis=1),
        jnp.concatenate([pair, pair], axis=0),
        preferred_element_type=F32,
    )
    small = jnp.dot(
        jnp.concatenate([left_high, left_low], axis=1),
        jnp.concatenate([low, high], axis=0),
        preferred_element_type=F32,
    )
    whole = (small + main[:, extent:]) + main[:, :extent]
    return [whole[i * extent : (i + 1) * extent] for i in range(len(lefts))]


def eye(extent, value):
    down = lax.broadcasted_iota(jnp.int32, (extent, extent), 0)
    across = lax.broadcasted_iota(jnp.int32, (extent, extent), 1)
    return jnp.where(down == across, jnp.broadcast_to(value, (extent, extent)), 0.0)


def scale_and_bound(samples, gram_peak, squares, size, average):
    target = squares / samples / size
    lift = shrink * target + ridge * average
    weight = (1.0 - shrink) / samples
    return weight, lift, weight * gram_peak + lift


def whiten_rows(block, turned, inner, squares, peak, size, average, out):
    samples = block.shape[0]
    weight, lift, bound = scale_and_bound(samples, peak, squares, size, average)
    inverse_bound = 1.0 / bound
    v = inner * (weight * inverse_bound)
    e = 1.0 - lift * inverse_bound
    c = jnp.ones_like(e)
    u = d = None
    for step in range(ITERS):
        lefts = [] if step == ITERS - 1 else [v] if step == 0 else [v, u]
        results = products(lefts + ([d] if step > 1 else []), v)
        if step == 0:
            d, u = eye(samples, -c), eye(samples, 2.0 * e) - v
        else:
            through = results[-1] if step > 1 else -v
            d = (1.0 + e) * d - c * u - through
            if lefts:
                u = 2.0 * e * u - results[1]
        if lefts:
            v = 2.0 * e * v - results[0]
        c = c * (1.0 + e)
        e = e * e
    mixed = sum(jnp.dot(piece, block, preferred_element_type=F32) for piece in reversed(thirds(d)))
    mixed = mixed * (weight * inverse_bound)
    width = block.shape[1]
    stacked = jnp.concatenate(thirds(mixed), axis=0)
    wide_turned = jnp.concatenate([turned] * 3, axis=1)
    inverse = jnp.dot(wide_turned, stacked, preferred_element_type=F32) * inverse_bound
    inverse = (inverse + eye(width, c * inverse_bound)).astype(BF16)
    out(jnp.dot(block, inverse, preferred_element_type=F32).astype(BF16))


def whiten_columns(block, gram_ref, current_ref, squares, peak, size, average, out):
    samples, width = block.shape
    weight, lift, bound = scale_and_bound(samples, peak, squares, size, average)
    gram_ref[...] = weight * gram_ref[...] + eye(width, lift)
    current_ref[...] = eye(width, 1.0 / bound)

    def sweep(i, carry):
        current = current_ref[...]
        product = jnp.dot(gram_ref[...], current, precision=HIGHEST, preferred_element_type=F32)
        current_ref[...] = jnp.dot(
            current, eye(width, jnp.full((1, 1), 2.0, F32)) - product, precision=HIGHEST, preferred_element_type=F32
        )
        return carry

    lax.fori_loop(0, ITERS, sweep, 0)
    out(jnp.dot(block, current_ref[...].astype(BF16), preferred_element_type=F32).astype(BF16))


def fused_kernel(
    samples_count,
    groups_count,
    entries,
    size_hbm,
    label_hbm,
    observed_hbm,
    result_ref,
    size_ref,
    label_ref,
    observed_ref,
    load_sem,
    sorted_ref,
    high_ref,
    turn_ref,
    place_ref,
    filled_ref,
    packed_ref,
    held_ref,
    done_ref,
    back_ref,
    energy_ref,
    group_ref,
    total_ref,
    all_ref,
    *rest,
):
    *work, group_send, group_recv, total_send, total_recv, out_send, out_recv, back_send, back_recv = rest
    me = lax.axis_index("samples")
    group = lax.axis_index("groups")
    _, slot_here, rows, width = packed_ref.shape
    samples = samples_count * rows
    slots = samples_count * slot_here
    tiles = sorted_ref.shape[0]
    parts = width // LANES
    unrolled = tiles * slots <= UNROLL_LIMIT
    order = sorted(range(1, samples_count), key=lambda k: abs(2 * k - samples_count))

    def ahead(k):
        return lax.rem(me + k, samples_count)

    def behind(k):
        return lax.rem(me + samples_count - k, samples_count)

    def copy(source, target, send, recv, sample, other):
        return pltpu.make_async_remote_copy(
            src_ref=source,
            dst_ref=target,
            send_sem=send,
            recv_sem=recv,
            device_id=(sample, other),
            device_id_type=MESH,
        )

    def columns(t):
        return pl.ds(t * LANES if isinstance(t, int) else pl.multiple_of(t * LANES, LANES), LANES)

    loads = [
        pltpu.make_async_copy(source, target, load_sem.at[i])
        for i, (source, target) in enumerate(
            ((label_hbm, label_ref), (observed_hbm, observed_ref), (size_hbm, size_ref))
        )
    ]
    for item in loads:
        item.start()
    barrier = pltpu.get_barrier_semaphore()
    for k in range(1, samples_count):
        pl.semaphore_signal(barrier, inc=1, device_id=(ahead(k), group), device_id_type=MESH)
    for k in range(1, groups_count):
        other = lax.rem(group + k, groups_count)
        pl.semaphore_signal(barrier, inc=1, device_id=(me, other), device_id_type=MESH)

    for item in loads:
        item.wait()

    first = group * slots
    slot = lax.broadcasted_iota(jnp.int32, (slots, LANES), 0)
    down = lax.broadcasted_iota(jnp.int32, (LANES, LANES), 0)
    across = lax.broadcasted_iota(jnp.int32, (LANES, LANES), 1)
    upto = (down <= across).astype(BF16)
    ones = jnp.ones((LANES, LANES), BF16)

    def compare(t):
        label = label_ref[pl.ds(t, 1), :] - first
        return (label == slot).astype(F32), (label < slot).astype(F32)

    def counts(equal, less):
        rank = jnp.dot(equal.astype(BF16), upto, preferred_element_type=F32) - 1.0
        count = jnp.dot(equal.astype(BF16), ones, preferred_element_type=F32)
        before = jnp.dot(less.astype(BF16), ones, preferred_element_type=F32)
        return rank, count, before

    if unrolled:
        pairs = [compare(t) for t in range(tiles)]
        stacked = counts(*(jnp.concatenate(items, axis=0) for items in zip(*pairs)))

    def sort_tile(t, carry):
        base, energy = carry
        if unrolled:
            equal = pairs[t][0]
            rank, count, before = (item[t * slots : (t + 1) * slots] for item in stacked)
        else:
            equal, less = compare(t)
            rank, count, before = counts(equal, less)
        local = jnp.sum(equal * (before + rank), axis=0, keepdims=True).astype(jnp.int32)
        whole = slot.astype(F32) * CMAX + base + rank
        place_ref[pl.ds(t, 1), :] = jnp.sum(equal * whole, axis=0, keepdims=True).astype(jnp.int32)
        block = observed_ref[:, columns(t)]
        choose = (down == local).astype(BF16)
        sorted_ref[t] = lax.dot_general(
            block, choose, (((1,), (1,)), ((), ())), preferred_element_type=F32
        )
        high_ref[t] = (base + count).astype(jnp.int32)
        turn_ref[t] = (before - base).astype(jnp.int32)
        wide = block.astype(F32)
        square = wide * wide
        for r in range(0, rows, 8):
            energy = energy + square[r : r + 8]
        return base + count, energy

    start = (jnp.zeros((slots, LANES), F32), jnp.zeros((8, LANES), F32))
    _, total = loop(tiles, sort_tile, start, unrolled)
    energy_ref[...] = total

    lane = lax.broadcasted_iota(jnp.int32, (rows, LANES), 1)

    def pack_slot(sample, h, target):
        c = sample * slot_here + h

        def add_tile(i, packed):
            t = tiles - 1 - i
            high = jnp.broadcast_to(high_ref[t, pl.ds(c, 1), :], (rows, LANES))
            turn = jnp.broadcast_to(turn_ref[t, pl.ds(c, 1), :], (rows, LANES))
            moved = lane_gather(sorted_ref[t], (lane + turn) & (LANES - 1))
            return tuple(
                jnp.where(lane + q * LANES < high, moved, packed[q])
                for q in range(parts)
            )

        zero = jnp.zeros((rows, LANES), F32)
        packed = loop(tiles, add_tile, (zero,) * parts, unrolled)
        for q in range(parts):
            target[:, q * LANES : (q + 1) * LANES] = packed[q].astype(BF16)

    group_copies = [
        copy(
            energy_ref,
            group_ref.at[k - 1],
            group_send.at[k - 1],
            group_recv.at[k - 1],
            me,
            lax.rem(group + k, groups_count),
        )
        for k in range(1, groups_count)
    ]
    out_copies = {
        k: copy(packed_ref.at[k], held_ref.at[k], out_send.at[k - 1], out_recv.at[k - 1], ahead(k), group)
        for k in order
    }
    total_copies = [
        copy(total_ref, all_ref.at[k - 1], total_send.at[k - 1], total_recv.at[k - 1], ahead(k), group)
        for k in order
    ]
    back_copies = [
        copy(done_ref.at[k], back_ref.at[me], back_send.at[k - 1], back_recv.at[me], behind(k), group)
        for k in order
    ]

    for k in order:
        for h in range(slot_here):
            pack_slot(ahead(k), h, packed_ref.at[k, h])
    pl.semaphore_wait(barrier, samples_count + groups_count - 2)
    for item in group_copies:
        item.start()
    for k in order:
        out_copies[k].start()
    for h in range(slot_here):
        pack_slot(me, h, held_ref.at[0, h])
    for item in group_copies:
        item.wait_recv()
    for k in range(groups_count - 1):
        total = total + group_ref[k]
    total_ref[...] = total
    for item in total_copies:
        item.start()
    for k in order:
        out_copies[k].wait_recv()

    average = None
    for h in range(slot_here):
        block = held_ref[:, h].reshape(samples, width)
        turned = block.T
        wide = block.astype(F32)
        squares = jnp.sum(jnp.sum(wide * wide, axis=0, keepdims=True), axis=1, keepdims=True)
        sums = jnp.zeros((1, width), F32)
        for r in range(0, width, LANES):
            part = jnp.dot(turned[r : r + LANES], block, preferred_element_type=F32)
            if work:
                work[0][r : r + LANES, :] = part
            sums = sums + jnp.sum(jnp.abs(part), axis=0, keepdims=True)
        peak = jnp.max(sums, axis=1, keepdims=True)
        if not work:
            inner = lax.dot_general(block, block, (((1,), (1,)), ((), ())), preferred_element_type=F32)
        if average is None:
            for item in total_copies:
                item.wait_recv()
            for k in range(samples_count - 1):
                total = total + all_ref[k]
            energy = jnp.sum(jnp.sum(total, axis=0, keepdims=True), axis=1, keepdims=True)
            average = energy / entries
        size = jnp.full((1, 1), size_ref[me * slot_here + h], jnp.int32).astype(F32)

        def out(value):
            done_ref[:, h] = value.reshape(samples_count, rows, width)

        if work:
            whiten_columns(block, work[0], work[1], squares, peak, size, average, out)
        else:
            whiten_rows(block, turned, inner, squares, peak, size, average, out)

    for item in back_copies:
        item.start()

    def fill(sample, source, opening):
        for h in range(slot_here):
            wide = [source[h, :, q * LANES : (q + 1) * LANES].astype(F32) for q in range(parts)]

            def fill_tile(t, carry):
                place = jnp.broadcast_to(place_ref[pl.ds(t, 1), :], (rows, LANES))
                index = place & (LANES - 1)
                tile = (place >> (LANES.bit_length() - 1)) - (sample * slot_here + h) * parts
                if opening and h == 0:
                    value = jnp.zeros((rows, LANES), F32)
                else:
                    value = filled_ref[t]
                for q in range(parts):
                    value = jnp.where(tile == q, lane_gather(wide[q], index), value)
                filled_ref[t] = value
                return carry

            loop(tiles, fill_tile, 0, unrolled)

    fill(me, done_ref.at[0], True)
    for k in reversed(order):
        copy(
            done_ref.at[k], back_ref.at[ahead(k)], back_send.at[k - 1], back_recv.at[ahead(k)], ahead(k), group
        ).wait_recv()
        fill(ahead(k), back_ref.at[ahead(k)], False)

    def finish(t, carry):
        result_ref[:, columns(t)] = filled_ref[t]
        return carry

    loop(tiles, finish, 0, unrolled)
    for item in group_copies + list(out_copies.values()) + total_copies + back_copies:
        item.wait_send()


def pieces(value):
    high = value.astype(BF16)
    return high, (value - high.astype(F32)).astype(BF16)


def stack_product(lefts, right):
    extent = right[0].shape[1]
    pair = jnp.concatenate(right, axis=1)
    left = jnp.concatenate([jnp.concatenate(item, axis=1) for item in lefts], axis=0)
    both = jnp.dot(left, jnp.concatenate([pair, pair], axis=0), preferred_element_type=F32)
    whole = both[:, extent:] + both[:, :extent]
    rows = right[0].shape[0]
    return [whole[i * rows : (i + 1) * rows] for i in range(len(lefts))]


def residual_series(gram, peak, box):
    extent = gram.shape[0]
    one = eye(extent, jnp.ones((1, 1), F32))
    positive = peak > 0.0
    unit = jnp.where(positive, 1.0 / jnp.where(positive, peak, 1.0), 0.0)
    first = one - gram * unit
    cut = pieces(first)
    (second,) = stack_product([cut], cut)
    cut_second = pieces(second)
    yield
    third, power = stack_product([cut, cut_second], cut_second)
    yield
    e = box[0]
    square = e * e
    count = 1.0 + e
    series = one * (count + square) + first * (e + square) + second * square
    total = (one + first) + (second + third)
    count = count * (1.0 + square)
    before, raised = e * square, square * square
    yield
    for _ in range(2):
        cut = pieces(power)
        power, through, more = stack_product([cut, pieces(series), pieces(total)], cut)
        series = series + through * raised + total * (before * count)
        total = total + more
        count = count * (1.0 + raised)
        before, raised = before * raised, raised * raised
        yield
    (through,) = stack_product([pieces(series)], pieces(power))
    yield series + through * raised + total * (before * count), count * (1.0 + raised)


def residual_powers(gram, peak):
    extent = gram.shape[0]
    one = eye(extent, jnp.ones((1, 1), F32))
    positive = peak > 0.0
    unit = jnp.where(positive, 1.0 / jnp.where(positive, peak, 1.0), 0.0)
    power = {1: one - gram * unit}
    cut = {1: pieces(power[1])}
    yield

    def extend(names, by):
        for name, value in zip(names, stack_product([cut[n - by] for n in names], cut[by])):
            power[name] = value
            cut[name] = pieces(value)

    extend([2], 1)
    yield
    extend([3, 4], 2)
    yield
    extend([5, 6, 7, 8], 4)
    total = {8: one + sum(power[i] for i in range(1, 8))}
    first = pieces(total[8])
    yield
    power[16], more = stack_product([cut[8], first], cut[8])
    total[16] = total[8] + more
    cut[16] = pieces(power[16])
    yield
    power[24], more = stack_product([cut[8], first], cut[16])
    total[24] = total[16] + more
    yield power, total


def powers_series(power, total, e):
    raised = {0: jnp.ones_like(e), 1: e}
    for i in (2, 3, 4, 5, 6, 7, 8):
        raised[i] = raised[i // 2] * raised[i - i // 2]
    raised[15] = raised[8] * raised[7]
    raised[16] = raised[8] * raised[8]
    raised[23] = raised[16] * raised[7]
    raised[24] = raised[16] * raised[8]
    tail = {7: raised[7]}
    for i in range(6, -1, -1):
        tail[i] = raised[i] + tail[i + 1]
    eight = tail[0]
    extent = power[1].shape[0]
    series = eye(extent, eight - raised[7])
    for i in range(1, 7):
        series = series + power[i] * (tail[i] - raised[7])
    spread = sum(power[i] * raised[i] for i in (8, 16, 24))
    rest = sum(total[i] * (eight * raised[i - 1]) for i in (8, 16, 24))
    (through,) = stack_product([pieces(spread)], pieces(series))
    whole = eight * (1.0 + raised[8]) * (1.0 + raised[16])
    return through + (series + rest), whole


def late_series(gram, peak, box):
    maker = residual_powers(gram, peak)
    for _ in range(5):
        next(maker)
        yield
    power, total = next(maker)
    yield
    yield powers_series(power, total, box[0])


def whiten_pair(leads, block, odd, sizes, flag_ref, same_ref, inverse_ref, share_total, wait_average, out):
    samples, width = block.shape
    turned = block.T
    second = block * odd.astype(BF16)
    first = block - second
    both = jnp.concatenate([first, second], axis=0)
    second_turned = turned * flag_ref[...]
    both_turned = jnp.concatenate([turned - second_turned, second_turned], axis=1)
    inner = jnp.dot(block, both_turned, preferred_element_type=F32)
    lines = [jnp.zeros((1, LANES), F32)] * (width // LANES)
    for r in range(0, width, LANES):
        part = jnp.abs(jnp.dot(both_turned[r : r + LANES], both[:, r:], preferred_element_type=F32))
        down = jnp.sum(part, axis=0, keepdims=True)
        for q in range(r, width, LANES):
            lines[q // LANES] = lines[q // LANES] + down[:, q - r : q - r + LANES]
        if r + LANES < width:
            right = sum(part[:, q - r : q - r + LANES] for q in range(r + LANES, width, LANES))
            lines[r // LANES] = lines[r // LANES] + jnp.sum(right.T, axis=0, keepdims=True)
    sums = jnp.concatenate(lines, axis=1)
    peaks = [jnp.max(sums * side, axis=1, keepdims=True) for side in (1.0 - odd, odd)]
    grams = [inner[:, :samples], inner[:, samples:]]
    traces = []
    for gram in grams:
        kept = gram * eye(samples, jnp.ones((1, 1), F32))
        traces.append(jnp.sum(jnp.sum(kept, axis=0, keepdims=True), axis=1, keepdims=True))
    boxes = [[], []]
    make = residual_series if leads else late_series
    makers = [make(gram, peak, box) for gram, peak, box in zip(grams, peaks, boxes)]
    for step in range(2 if leads else 6):
        for maker in makers:
            next(maker)
        if leads and step == 0:
            share_total()
    average = wait_average()
    weight = (1.0 - shrink) / samples
    inverse_bounds = []
    for peak, trace, size, box in zip(peaks, traces, sizes, boxes):
        lift = shrink * (trace / samples / size) + ridge * average
        inverse_bound = 1.0 / (weight * peak + lift)
        box.append(weight * peak * inverse_bound)
        inverse_bounds.append(inverse_bound)
    for _ in range(4 if leads else 1):
        found = [next(maker) for maker in makers]
    middles = [piece for middle, _ in found for piece in pieces(middle)]
    wholes = [whole for _, whole in found]
    factors = [weight * inverse_bound for inverse_bound in inverse_bounds]

    def by_side(values):
        return jnp.where(odd > 0.5, values[1], values[0])

    mixed = jnp.dot(
        jnp.concatenate(middles, axis=1),
        jnp.concatenate([first, first, second, second], axis=0),
        preferred_element_type=F32,
    )
    mixed = mixed * (-by_side(factors))
    stacked = jnp.concatenate(pieces(mixed), axis=0)
    scale = by_side(inverse_bounds)
    peak_line = by_side(wholes)
    wide_turned = jnp.concatenate([turned, turned], axis=1)
    for r in range(0, width, LANES):
        part = jnp.dot(wide_turned[r : r + LANES], stacked[:, r:], preferred_element_type=F32)
        line = eye(LANES, jnp.ones((1, 1), F32)) * peak_line[:, r : r + LANES]
        for q in range(r, width, LANES):
            value = part[:, q - r : q - r + LANES]
            if q == r:
                value = value + line
            value = (value * scale[:, q : q + LANES]).astype(BF16)
            value = value * same_ref[r : r + LANES, q : q + LANES]
            inverse_ref[r : r + LANES, q : q + LANES] = value
            if q > r:
                inverse_ref[q : q + LANES, r : r + LANES] = value.T
    out(jnp.dot(block, inverse_ref[...], preferred_element_type=F32).astype(BF16))


def pair_kernel(
    samples_count,
    groups_count,
    entries,
    size_hbm,
    label_hbm,
    observed_hbm,
    result_ref,
    size_ref,
    label_ref,
    observed_ref,
    load_sem,
    sorted_ref,
    side_ref,
    high_ref,
    turn_ref,
    place_ref,
    packed_ref,
    held_ref,
    odd_ref,
    flag_ref,
    same_ref,
    inverse_ref,
    done_ref,
    back_ref,
    energy_ref,
    all_ref,
    total_ref,
    total_in_ref,
    energy_send,
    energy_recv,
    total_send,
    total_recv,
    out_send,
    out_recv,
    back_send,
    back_recv,
):
    me = lax.axis_index("samples")
    group = lax.axis_index("groups")
    pairs, rows, width = packed_ref.shape
    tiles = sorted_ref.shape[0]
    table_rows = high_ref.shape[1]
    parts = width // LANES
    opening = samples_count // 4
    mine = jnp.clip(me - opening, 0, pairs - 1)
    inverts = (me >= opening) & (me < opening + pairs)
    hub_group = group == 0
    later = jnp.minimum(group, 1)
    number = group * samples_count + me
    devices = samples_count * groups_count

    def copy(source, target, send, recv, sample, other):
        return pltpu.make_async_remote_copy(
            src_ref=source,
            dst_ref=target,
            send_sem=send,
            recv_sem=recv,
            device_id=(sample, other),
            device_id_type=MESH,
        )

    def signal(sample, other):
        pl.semaphore_signal(barrier, inc=1, device_id=(sample, other), device_id_type=MESH)

    loads = [
        pltpu.make_async_copy(source, target, load_sem.at[i])
        for i, (source, target) in enumerate(
            ((label_hbm, label_ref), (observed_hbm, observed_ref), (size_hbm, size_ref))
        )
    ]
    for item in loads:
        item.start()
    barrier = pltpu.get_barrier_semaphore()

    @pl.when(inverts)
    def _():
        for k in range(samples_count - 1):
            signal(k + (me <= k).astype(jnp.int32), group)

    @pl.when(inverts & hub_group)
    def _():
        for j in range(1, groups_count):
            for k in range(samples_count):
                signal(lax.rem(me + k, samples_count), lax.rem(group + j, groups_count))

    for item in loads:
        item.wait()

    slots = 2 * pairs
    first = group * slots
    slot = lax.broadcasted_iota(jnp.int32, (table_rows, LANES), 0)
    down = lax.broadcasted_iota(jnp.int32, (LANES, LANES), 0)
    across = lax.broadcasted_iota(jnp.int32, (LANES, LANES), 1)
    upto = (down <= across).astype(BF16)
    ones = jnp.ones((LANES, LANES), BF16)
    energy = jnp.zeros((8, LANES), F32)
    equals, lesses, blocks, sides = [], [], [], []
    for t in range(tiles):
        block = observed_ref[:, t * LANES : (t + 1) * LANES]
        wide = block.astype(F32)
        square = wide * wide
        for r in range(0, rows, 8):
            energy = energy + square[r : r + 8]
        label = label_ref[pl.ds(t, 1), :] - first
        pair = label >> 1
        equals.append((pair == slot).astype(F32))
        lesses.append((pair < slot).astype(F32))
        side = jnp.broadcast_to((label & 1).astype(F32), (rows, LANES)).astype(BF16)
        blocks.append(jnp.concatenate([block, side], axis=0))
    energy_ref[0] = jnp.sum(energy, axis=0, keepdims=True)
    all_ref[number] = energy_ref[0]
    equal_all = jnp.concatenate(equals, axis=0).astype(BF16)
    less_all = jnp.concatenate(lesses, axis=0).astype(BF16)
    ranks = jnp.dot(equal_all, upto, preferred_element_type=F32) - 1.0
    counts = jnp.dot(equal_all, ones, preferred_element_type=F32)
    befores = jnp.dot(less_all, ones, preferred_element_type=F32)
    base = jnp.zeros((table_rows, LANES), F32)
    for t in range(tiles):
        span = slice(t * table_rows, (t + 1) * table_rows)
        rank, count, before, equal = ranks[span], counts[span], befores[span], equals[t]
        local = jnp.sum(equal * (before + rank), axis=0, keepdims=True).astype(jnp.int32)
        whole = slot.astype(F32) * width + base + rank
        place_ref[pl.ds(t, 1), :] = jnp.sum(equal * whole, axis=0, keepdims=True).astype(jnp.int32)
        choose = (down == local).astype(BF16)
        ordered = lax.dot_general(blocks[t], choose, (((1,), (1,)), ((), ())), preferred_element_type=F32)
        sorted_ref[t] = ordered[:rows]
        side_ref[t] = ordered[rows : rows + 8]
        high_ref[t] = (base + count).astype(jnp.int32)
        turn_ref[t] = (before - base).astype(jnp.int32)
        base = base + count

    lane = lax.broadcasted_iota(jnp.int32, (rows, LANES), 1)

    def reach(t):
        return range(max(0, parts - tiles + t), min(parts, t + 1))

    def pack(c, source, height):
        packed = [jnp.zeros((height, LANES), F32)] * parts
        place = lane[:height]
        for t in reversed(range(tiles)):
            high = jnp.broadcast_to(high_ref[t, pl.ds(c, 1), :], (height, LANES))
            turn = jnp.broadcast_to(turn_ref[t, pl.ds(c, 1), :], (height, LANES))
            moved = lane_gather(source[t], (place + turn) & (LANES - 1))
            for q in reach(t):
                packed[q] = jnp.where(place + q * LANES < high, moved, packed[q])
        return packed

    for p in range(pairs):
        for q, value in enumerate(pack(p, sorted_ref, rows)):
            packed_ref[p, :, q * LANES : (q + 1) * LANES] = value.astype(BF16)

    near_half = me < opening + pairs // 2
    far_first = [jnp.where(near_half, pairs - 1 - k, k) for k in range(pairs)]
    out_copies = [
        copy(packed_ref.at[p], held_ref.at[me], out_send.at[k], out_recv.at[me], opening + p, group)
        for k, p in enumerate(far_first)
    ]
    hubs = [(opening + p, 0) for p in range(pairs)]
    energy_copies = [
        copy(energy_ref.at[0], all_ref.at[number], energy_send.at[i], energy_recv, sample, other)
        for i, (sample, other) in enumerate(hubs)
    ]

    def elsewhere(sample, other=None):
        away = me != sample
        return away if other is None else away | (group != other)

    pl.semaphore_wait(barrier, (1 + later) * pairs - inverts.astype(jnp.int32))
    for item, hub in zip(energy_copies, hubs):
        pl.when(elsewhere(*hub))(item.start)
    for p, item in zip(far_first, out_copies):
        pl.when(elsewhere(opening + p))(item.start)

    total_copies = [
        copy(total_ref, total_in_ref, total_send.at[g - 1], total_recv, me, g) for g in range(1, groups_count)
    ]

    @pl.when(inverts)
    def _():
        held_ref[me] = packed_ref[mine]
        odd = jnp.concatenate(pack(mine, side_ref, 8), axis=1)
        odd_ref[...] = odd
        odd_turned = jnp.concatenate([odd] * (LANES // 8), axis=0).T
        flag_ref[...] = odd_turned.astype(BF16)
        for r in range(0, width, LANES):
            for q in range(0, width, LANES):
                same = odd_turned[r : r + LANES] == jnp.broadcast_to(odd[:1, q : q + LANES], (LANES, LANES))
                same_ref[r : r + LANES, q : q + LANES] = same.astype(F32).astype(BF16)
        for k in range(1, samples_count):
            other = lax.rem(me + k, samples_count)
            copy(
                packed_ref.at[0], held_ref.at[other], out_send.at[0], out_recv.at[other], me, group
            ).wait_recv()

        def share_total():
            rest = all_ref.at[pl.ds(0, devices - 1)]
            copy(rest, rest, energy_send.at[0], energy_recv, me, group).wait_recv()
            total = jnp.sum(all_ref[...], axis=0)
            total_in_ref[...] = total
            total_ref[...] = total
            for item in total_copies:
                item.start()

        def wait_average(leads):
            if not leads:
                total_copies[0].wait_recv()
            return jnp.sum(total_in_ref[...], axis=1, keepdims=True) / entries

        def out(value):
            done_ref[...] = value.reshape(samples_count, rows, width)

        sizes = [
            jnp.full((1, 1), size_ref[2 * mine + h], jnp.int32).astype(F32) for h in range(2)
        ]
        def invert(leads):
            block = held_ref[...].reshape(samples_count * rows, width)
            whiten_pair(
                leads,
                block,
                odd_ref[:1],
                sizes,
                flag_ref,
                same_ref,
                inverse_ref,
                share_total,
                functools.partial(wait_average, leads),
                out,
            )

        pl.when(hub_group)(functools.partial(invert, True))
        pl.when(group != 0)(functools.partial(invert, False))
        for k in range(samples_count - 1):
            other = k + (me <= k).astype(jnp.int32)
            copy(
                done_ref.at[other], back_ref.at[mine], back_send.at[k], back_recv.at[mine], other, group
            ).start()
        back_ref[mine] = done_ref[me]

    for k in range(pairs):
        p = jnp.where(me < opening + pairs // 2, k, pairs - 1 - k)

        @pl.when(elsewhere(opening + p))
        def _():
            copy(
                done_ref.at[0], back_ref.at[p], back_send.at[0], back_recv.at[p], opening + p, group
            ).wait_recv()

        wide = [back_ref[p, :, q * LANES : (q + 1) * LANES].astype(F32) for q in range(parts)]
        for t in range(tiles):
            place = jnp.broadcast_to(place_ref[pl.ds(t, 1), :], (rows, LANES))
            index = place & (LANES - 1)
            tile = (place >> (LANES.bit_length() - 1)) - p * parts
            if k == 0:
                value = jnp.zeros((rows, LANES), F32)
            else:
                value = result_ref[:, t * LANES : (t + 1) * LANES]
            for q in reach(t):
                value = jnp.where(tile == q, lane_gather(wide[q], index), value)
            result_ref[:, t * LANES : (t + 1) * LANES] = value

    for item, hub in zip(energy_copies, hubs):
        pl.when(elsewhere(*hub))(item.wait_send)
    for p, item in zip(far_first, out_copies):
        pl.when(elsewhere(opening + p))(item.wait_send)

    @pl.when(inverts & hub_group)
    def _():
        for item in total_copies:
            item.wait_send()


    @pl.when(inverts)
    def _():
        for k in range(samples_count - 1):
            other = k + (me <= k).astype(jnp.int32)
            copy(
                done_ref.at[other], back_ref.at[mine], back_send.at[k], back_recv.at[mine], other, group
            ).wait_send()


def paired(observed, labels, comp_sizes, samples_count, groups_count):
    rows, width = observed.shape
    pairs = comp_sizes.shape[0] // 2
    pair_width = width // pairs
    tiles = width // LANES
    devices = samples_count * groups_count
    table_rows = -(-pairs // 8) * 8
    kind = pltpu.SemaphoreType.DMA
    table = pltpu.VMEM((tiles, table_rows, LANES), jnp.int32)
    square = pltpu.VMEM((pair_width, pair_width), BF16)
    blocks = pltpu.VMEM((samples_count, rows, pair_width), BF16)
    kept = pltpu.VMEM((pairs, rows, pair_width), BF16)
    line = pltpu.VMEM((1, LANES), F32)
    return pl.pallas_call(
        functools.partial(
            pair_kernel, samples_count, groups_count, float(samples_count * rows * width * groups_count)
        ),
        out_shape=pltpu.VMEM((rows, width), F32),
        in_specs=[pl.BlockSpec(memory_space=pltpu.HBM)] * 3,
        out_specs=VMEM,
        scratch_shapes=[
            pltpu.SMEM(comp_sizes.shape, jnp.int32),
            pltpu.VMEM((tiles, LANES), jnp.int32),
            pltpu.VMEM((rows, width), BF16),
            kind((3,)),
            pltpu.VMEM((tiles, rows, LANES), F32),
            pltpu.VMEM((tiles, 8, LANES), F32),
            table,
            table,
            pltpu.VMEM((tiles, LANES), jnp.int32),
            kept,
            blocks,
            pltpu.VMEM((8, pair_width), F32),
            pltpu.VMEM((pair_width, LANES), BF16),
            square,
            square,
            blocks,
            kept,
            pltpu.VMEM((1, 1, LANES), F32),
            pltpu.VMEM((devices, 1, LANES), F32),
            line,
            line,
            kind((pairs,)),
            kind,
            kind((groups_count - 1,)),
            kind,
            kind((pairs,)),
            kind((samples_count,)),
            kind((samples_count,)),
            kind((pairs,)),
        ],
        compiler_params=pltpu.CompilerParams(
            collective_id=0, has_side_effects=True, vmem_limit_bytes=56 * 2**20
        ),
        name="whiten",
    )(comp_sizes, labels.reshape(tiles, LANES), observed).astype(BF16)


def pairs_fit(rows, width, slots, samples_count, groups_count):
    return (
        slots == samples_count
        and samples_count % 4 == 0
        and groups_count > 1
        and rows * samples_count < CMAX
        and (2 * width // slots) % LANES == 0
        and rows % 16 == 0
    )


def body(observed, labels, comp_sizes):
    rows, width = observed.shape
    slots = comp_sizes.shape[0]
    samples_count = lax.axis_size("samples")
    groups_count = lax.axis_size("groups")
    if pairs_fit(rows, width, slots, samples_count, groups_count):
        return paired(observed, labels, comp_sizes, samples_count, groups_count)
    slot_here = slots // samples_count
    tiles = width // LANES
    samples = rows * samples_count
    kind = pltpu.SemaphoreType.DMA
    table = pltpu.VMEM((tiles, slots, LANES), jnp.int32)
    wide_tiles = pltpu.VMEM((tiles, rows, LANES), F32)
    blocks = pltpu.VMEM((samples_count, slot_here, rows, CMAX), BF16)
    work = [pltpu.VMEM((CMAX, CMAX), F32)] * 2 if samples >= CMAX else []
    return pl.pallas_call(
        functools.partial(
            fused_kernel, samples_count, groups_count, float(samples * width * groups_count)
        ),
        out_shape=pltpu.VMEM((rows, width), F32),
        in_specs=[pl.BlockSpec(memory_space=pltpu.HBM)] * 3,
        out_specs=VMEM,
        scratch_shapes=[
            pltpu.SMEM(comp_sizes.shape, jnp.int32),
            pltpu.VMEM((tiles, LANES), jnp.int32),
            pltpu.VMEM((rows, width), BF16),
            kind((3,)),
            wide_tiles,
            table,
            table,
            pltpu.VMEM((tiles, LANES), jnp.int32),
            wide_tiles,
            blocks,
            blocks,
            blocks,
            blocks,
            pltpu.VMEM((8, LANES), F32),
            pltpu.VMEM((groups_count - 1, 8, LANES), F32),
            pltpu.VMEM((8, LANES), F32),
            pltpu.VMEM((samples_count - 1, 8, LANES), F32),
            *work,
            kind((groups_count - 1,)),
            kind((groups_count - 1,)),
            kind((samples_count - 1,)),
            kind((samples_count - 1,)),
            kind((samples_count - 1,)),
            kind((samples_count - 1,)),
            kind((samples_count - 1,)),
            kind((samples_count,)),
        ],
        compiler_params=pltpu.CompilerParams(
            collective_id=0, has_side_effects=True, vmem_limit_bytes=56 * 2**20
        ),
        name="whiten",
    )(comp_sizes, labels.reshape(tiles, LANES), observed).astype(BF16)


def solution(mesh):
    return jax.shard_map(
        body,
        mesh=mesh,
        in_specs=(P("samples", "groups"), P("groups"), P("groups")),
        out_specs=P("samples", "groups"),
        check_vma=False,
    )
```
